32 devices in a mesh: dp: 8 (over z, x), cls: 4 (over y, core).
Axes of the slice: x: 2, y: 2, z: 4, core: 2. Of those that a mesh axis runs over, the one named last changes fastest.
Arguments:
- embeddings: bfloat16 [24576, 768], P('dp'), may hold values from -6 to 6
- labels: int32 [24576], P('dp'), may hold values from 0 to 2751, as said below
- row_count: int32 [8], P('dp'), may hold values from 768 to 3072
Outputs:
- class_means: float32 [2752, 768], P(('dp', 'cls'))
- prototypes: float32 [2752, 768], P(('dp', 'cls'))
- similarity: float32 [24576], P('dp')
The draws below stay inside these ranges and needn't reach their ends.
Inputs may be any that keep to these rules, and one draw needn't show every extreme that they name: Rows of index i of dp at or beyond row_count[i] are padding. `labels`: classes c and c' belong to the same block when c // 86 == c' // 86; block b belongs to index b mod 4 of cls. The rows of one index of dp name at most 16 distinct classes of any one block. Some block has exactly 16 of its classes named by the rows of every index of dp. The rows of some index of dp name exactly 16 classes of every block of some index of cls.
All inputs are finite; a program needn't handle non-finite values.
Results may differ from the reference program's by a relative error of at most 0.0017.
Values sent between devices are 32-bit elements; how exact they have to be, the bound alone decides.
No kernel may reach another device: no remote copies, remote signals or barrier semaphores. Data moves between devices by JAX's collectives and lax.ppermute only.
A program may use at most 64 MiB of HBM per device.

```python
import jax
import jax.numpy as jnp
from jax import lax

D = 768
CLS_DEV = 86
SLOTS = 16
ROWS_DEV = 3072
CLASSES = 2752
ROWS = 24576
N_DP = 8


def draw_labels(key, part):
    blocks = ROWS // ROWS_DEV
    owners = CLASSES // CLS_DEV
    group_count = owners // blocks
    keys = jax.random.split(jax.random.fold_in(key, 17), 7)
    class_iota = jnp.arange(CLS_DEV, dtype=jnp.int32)
    scores = jax.random.randint(keys[0], (blocks, owners, CLS_DEV), 0, 1 << 20) * CLS_DEV + class_iota
    allowed = jnp.argsort(scores, axis=2)[:, :, :SLOTS].astype(jnp.int32)
    owner_scores = jax.random.randint(keys[1], (owners,), 0, 1 << 20) * owners + jnp.arange(owners, dtype=jnp.int32)
    owner_order = jnp.argsort(owner_scores).astype(jnp.int32)
    first_pick = jax.random.randint(keys[2], (blocks, ROWS_DEV), 0, owners)
    second_pick = jax.random.randint(keys[3], (blocks, ROWS_DEV), 0, owners)
    owner_rank = jnp.minimum(first_pick, second_pick).astype(jnp.int32)
    slot_first = jax.random.randint(keys[4], (blocks, ROWS_DEV), 0, SLOTS)
    slot_second = jax.random.randint(keys[5], (blocks, ROWS_DEV), 0, SLOTS)
    slot = jnp.minimum(slot_first, slot_second).astype(jnp.int32)
    position = jnp.broadcast_to(jnp.arange(ROWS_DEV, dtype=jnp.int32)[None, :], (blocks, ROWS_DEV))
    block_index = jnp.broadcast_to(jnp.arange(blocks, dtype=jnp.int32)[:, None], (blocks, ROWS_DEV))
    forced = position < SLOTS
    owner_rank = jnp.where(forced, 0, owner_rank)
    slot = jnp.where(forced, position, slot)
    chosen_owner = owner_order[owner_rank].astype(jnp.int32)
    full_sender = jax.random.randint(keys[6], (), 0, blocks).astype(jnp.int32)
    base_group = (owner_order[0] % group_count).astype(jnp.int32)
    widened = (block_index == full_sender) & (position < blocks * SLOTS)
    wide_owner = (base_group + group_count * (position // SLOTS)).astype(jnp.int32)
    chosen_owner = jnp.where(widened, wide_owner, chosen_owner).astype(jnp.int32)
    slot = jnp.where(widened, position % SLOTS, slot).astype(jnp.int32)
    local_class = allowed[block_index, chosen_owner, slot]
    labels = chosen_owner * CLS_DEV + local_class
    return labels.reshape(ROWS).astype(jnp.int32)


def set_ends(entries, key, smallest, largest):
    place = [jax.random.randint(jax.random.fold_in(key, axis), (), 0, length) for axis, length in enumerate(entries.shape)]
    widest = entries.shape.index(max(entries.shape))
    neighbour = place[:widest] + [(place[widest] + 1) % entries.shape[widest]] + place[widest + 1:]
    return entries.at[tuple(place)].set(smallest).at[tuple(neighbour)].set(largest)


def level_of(stream_key, shape, cuts, smallest, top_value):
    gain, own = 1.0, jax.random.fold_in(stream_key, 6)
    for axis_at, shards_of in cuts:
        heights = jnp.exp(jax.random.uniform(jax.random.fold_in(own, axis_at), (shards_of,), jnp.float32, smallest / len(cuts), top_value / len(cuts)))
        gain = gain * jnp.repeat(heights, shape[axis_at] // shards_of).reshape([-1 if axis == axis_at else 1 for axis in range(len(shape))])
    return gain


def bell_draw(rng, extent, deviation, reach, cuts=(), held_as=jnp.bfloat16):
    array = jax.random.normal(rng, extent, jnp.float32) * deviation
    if len(cuts) > 0:
        array = level_of(rng, extent, cuts, -0.22, 0.18) * array
    return jnp.clip(array, min=-reach, max=reach).astype(held_as)


def setup_inputs(seed: int = 0) -> dict:
    splits = jax.random.split(jax.random.key(seed), 4)
    embeddings = bell_draw(splits[0], (ROWS, D), 1.0, 6.0, ((0, 8),))
    labels = draw_labels(jax.random.fold_in(splits[3], 71), 0)
    row_count = set_ends(jax.random.randint(splits[2], (N_DP,), max(ROWS_DEV // 4, N_DP * SLOTS), ROWS_DEV + 1), jax.random.fold_in(splits[2], 1), max(ROWS_DEV // 4, N_DP * SLOTS), ROWS_DEV).astype(jnp.int32)
    return dict(embeddings=embeddings, labels=labels, row_count=row_count)


epsilon = 1e-06
sharpness = 4.0

def normalize(matrix):
    return matrix / jnp.sqrt(lax.optimization_barrier(jnp.sum(matrix * matrix, axis=1, keepdims=True)) + epsilon)

def reference(embeddings, labels, row_count):
    row_total = embeddings.shape[0]
    position = jnp.arange(row_total, dtype=jnp.int32)
    owner = (position // ROWS_DEV).astype(jnp.int32)
    alive = (position % ROWS_DEV < row_count[owner]).astype(jnp.float32)
    features = embeddings.astype(jnp.float32)
    class_sums = jax.ops.segment_sum(features * alive[:, None], labels, num_segments=CLASSES)
    counts = jax.ops.segment_sum(alive, labels, num_segments=CLASSES)
    class_means = class_sums / jnp.maximum(counts, 1.0)[:, None]
    unit_rows = normalize(class_means)
    lengths = jnp.sqrt(lax.optimization_barrier(jnp.sum(features * features, axis=1)) + epsilon)
    similarity = alive * lax.optimization_barrier(jnp.sum(features * unit_rows[labels], axis=1)) / lengths
    weight = (alive * jnp.exp(sharpness * (similarity - 1.0))).astype(jnp.bfloat16).astype(jnp.float32)
    weighted = jax.ops.segment_sum(features * weight[:, None], labels, num_segments=CLASSES)
    prototypes = normalize(weighted)
    return (class_means, prototypes, similarity)
```

```python
import functools

import jax
import jax.numpy as jnp
from jax import lax
from jax.experimental import pallas as pl
from jax.experimental.pallas import tpu as pltpu
from jax.sharding import PartitionSpec as P

CLS_DEV = 86
SLOTS = 16
LANES = 128
CLS_PAD = 96

epsilon = 1e-06
sharpness = 4.0

VMEM = pl.BlockSpec(memory_space=pltpu.VMEM)
SMEM = pl.BlockSpec(memory_space=pltpu.SMEM)
VMEM_LIMIT = 24 * 1024 * 1024


def dot(a, b, dims):
    return lax.dot_general(a, b, (dims, ((), ())), preferred_element_type=jnp.float32)


def split2(x):
    hi = x.astype(jnp.bfloat16)
    lo = (x - hi.astype(jnp.float32)).astype(jnp.bfloat16)
    return hi, lo


def split3(x):
    hi = x.astype(jnp.bfloat16)
    rest = x - hi.astype(jnp.float32)
    mid, lo = split2(rest)
    return hi, mid, lo


def flags(mask, dtype=jnp.bfloat16):
    return jnp.where(mask, 1.0, 0.0).astype(dtype)


def iota(shape, axis):
    return lax.broadcasted_iota(jnp.int32, shape, axis).astype(jnp.float32)


def put_slots(ref, rows):
    pieces = rows.shape[1] // LANES
    for owner in range(rows.shape[0] // SLOTS):
        for piece in range(pieces):
            ref[owner, piece * SLOTS:(piece + 1) * SLOTS, :] = rows[
                owner * SLOTS:(owner + 1) * SLOTS, piece * LANES:(piece + 1) * LANES
            ]


def get_slots(ref, pieces):
    rows = []
    for owner in range(ref.shape[0]):
        rows.append(
            jnp.concatenate(
                [ref[owner, piece * SLOTS:(piece + 1) * SLOTS, :] for piece in range(pieces)], axis=1
            )
        )
    return jnp.concatenate(rows, axis=0)


def sums_kernel(group_count, place_ref, label_ref, rows_ref, out_ref, slot_ref):
    owner_count = out_ref.shape[0]
    slot_total = owner_count * SLOTS
    row_total, width = rows_ref.shape
    pieces = width // LANES
    my_group, my_owner, live = place_ref[0], place_ref[1], place_ref[2]
    label = label_ref[...].astype(jnp.float32)
    block = jnp.floor((label + 0.5) * (1.0 / CLS_DEV))
    inner = label - block * CLS_DEV
    owner = jnp.floor((block + 0.5) * (1.0 / group_count))
    group = block - owner * group_count
    position = lax.broadcasted_iota(jnp.int32, (1, row_total), 1)
    owned = (group == my_group.astype(jnp.float32)) & (position < live)
    owner = jnp.where(owned, owner, -1.0)
    owner_pad = max(owner_count, 16)
    by_owner = iota((owner_pad, row_total), 0) == owner
    by_class = flags(iota((LANES, row_total), 0) == inner)
    counts = dot(flags(by_owner), by_class, ((1,), (1,)))
    present = counts > 0
    upto = flags(iota((LANES, LANES), 0) <= iota((LANES, LANES), 1))
    rank = dot(flags(present), upto, ((1,), (0,))) - 1.0
    slot = jnp.where(present, rank, -1.0)
    row_slots = dot(slot.astype(jnp.bfloat16), by_class, ((1,), (0,)))
    row_slot = jnp.sum(jnp.where(by_owner, row_slots, 0.0), axis=0, keepdims=True)
    where_to = jnp.where(owned, owner * SLOTS + row_slot, -1.0)
    slot_ref[...] = where_to
    onehot = flags(iota((slot_total, row_total), 0) == where_to)
    put_slots(out_ref, dot(onehot, rows_ref[...], ((1,), (0,))))
    class_at = iota((owner_pad, LANES), 1)
    lane = lax.broadcasted_iota(jnp.int32, (owner_pad, slot_total), 1) - my_owner * SLOTS
    ids = jnp.zeros((owner_pad, slot_total), jnp.float32)
    tally = jnp.zeros((owner_pad, slot_total), jnp.float32)
    for s in range(SLOTS):
        hit = slot == s
        chosen = jnp.sum(jnp.where(hit, class_at + 1.0, 0.0), axis=1, keepdims=True) - 1.0
        number = jnp.sum(jnp.where(hit, counts, 0.0), axis=1, keepdims=True)
        ids = jnp.where(lane == s, chosen, ids)
        tally = jnp.where(lane == s, number, tally)
    sub = lax.broadcasted_iota(jnp.int32, (8, LANES), 0)
    for o in range(owner_count):
        for t in range(slot_total // LANES):
            lanes = slice(t * LANES, (t + 1) * LANES)
            tile = jnp.where(sub == 0, ids[o:o + 1, lanes], jnp.where(sub == 1, tally[o:o + 1, lanes], 0.0))
            base = pieces * SLOTS + 8 * t
            out_ref[o, base:base + 8, :] = tile


def means_kernel(got_ref, means_ref, back_ref, ids_ref):
    owner_count = got_ref.shape[0]
    slot_total = owner_count * SLOTS
    width = means_ref.shape[1]
    pieces = width // LANES
    metas = []
    for t in range(slot_total // LANES):
        base = pieces * SLOTS + 8 * t
        meta = got_ref[0, base:base + 8, :]
        for o in range(1, owner_count):
            meta = meta + got_ref[o, base:base + 8, :]
        metas.append(meta)
    meta = jnp.concatenate(metas, axis=1)
    ids = meta[0:1, :]
    ids_ref[...] = ids
    match = iota((CLS_PAD, slot_total), 0) == ids
    counts = jnp.sum(jnp.where(match, meta[1:2, :], 0.0), axis=1, keepdims=True)
    onehot = flags(match)
    sums = sum(dot(onehot, part, ((1,), (0,))) for part in split3(get_slots(got_ref, pieces)))
    means = sums / jnp.maximum(counts, 1.0)
    means_ref[...] = means[:means_ref.shape[0]]
    unit = means / jnp.sqrt(jnp.sum(means * means, axis=1, keepdims=True) + epsilon)
    put_slots(back_ref, sum(dot(onehot, part, ((0,), (0,))) for part in split2(unit)))


def lengths_kernel(rows_ref, out_ref):
    row_total, width = rows_ref.shape
    tile = min(512, row_total)
    ones = jnp.ones((16, width), jnp.bfloat16)
    for t in range(row_total // tile):
        features = rows_ref[t * tile:(t + 1) * tile, :].astype(jnp.float32)
        hi, lo = split2(features * features)
        total = dot(ones, hi, ((1,), (1,))) + dot(ones, lo, ((1,), (1,)))
        out_ref[:, t * tile:(t + 1) * tile] = jnp.sqrt(total[0:1] + epsilon)


def weigh_kernel(unit_ref, rows_ref, slot_ref, length_ref, out_ref, sim_ref, acc_ref):
    row_total, width = rows_ref.shape
    slot_total = out_ref.shape[0] * SLOTS
    units = jnp.concatenate(split2(get_slots(unit_ref, width // LANES)), axis=0)
    tile = min(512, row_total)
    for t in range(row_total // tile):
        part = slice(t * tile, (t + 1) * tile)
        rows = rows_ref[part, :]
        products = dot(units, rows, ((1,), (1,)))
        where_to = slot_ref[:, part]
        hit = iota((slot_total, tile), 0) == where_to
        product = jnp.sum(
            jnp.where(hit, products[:slot_total] + products[slot_total:], 0.0), axis=0, keepdims=True
        )
        owned = where_to >= 0
        similarity = jnp.where(owned, product / length_ref[:, part], 0.0)
        sim_ref[:, part] = similarity
        weight = jnp.exp(sharpness * (similarity - 1.0))
        weights = jnp.where(hit, weight, 0.0).astype(jnp.bfloat16)
        weighted = dot(weights, rows, ((1,), (0,)))
        if t == 0:
            acc_ref[...] = weighted
        else:
            acc_ref[...] += weighted
    put_slots(out_ref, acc_ref[...])


def prototypes_kernel(got_ref, ids_ref, out_ref):
    slot_total = got_ref.shape[0] * SLOTS
    onehot = flags(iota((CLS_PAD, slot_total), 0) == ids_ref[...])
    rows = get_slots(got_ref, out_ref.shape[1] // LANES)
    weighted = sum(dot(onehot, part, ((1,), (0,))) for part in split3(rows))
    unit = weighted / jnp.sqrt(jnp.sum(weighted * weighted, axis=1, keepdims=True) + epsilon)
    out_ref[...] = unit[:out_ref.shape[0]]


def call(kernel, ins, outs, name, scratch=(), cost=None):
    return pl.pallas_call(
        kernel,
        in_specs=ins,
        out_specs=[VMEM] * len(outs),
        out_shape=[jax.ShapeDtypeStruct(shape, jnp.float32) for shape in outs],
        scratch_shapes=list(scratch),
        compiler_params=pltpu.CompilerParams(vmem_limit_bytes=VMEM_LIMIT),
        cost_estimate=cost,
        name=name,
    )


def exchange(payload):
    return lax.all_to_all(payload, "dp", split_axis=0, concat_axis=0, tiled=True)


def shards(embeddings, labels, row_count):
    row_total, width = embeddings.shape
    group_count = lax.axis_size("cls")
    owner_count = lax.axis_size("dp")
    slot_total = owner_count * SLOTS
    pieces = width // LANES
    slot_rows = pieces * SLOTS
    meta_rows = 8 * (slot_total // LANES)
    place = jnp.stack([lax.axis_index("cls"), lax.axis_index("dp"), row_count[0]]).astype(jnp.int32)
    payload, where_to = call(
        functools.partial(sums_kernel, group_count),
        [SMEM, VMEM, VMEM],
        [(owner_count, slot_rows + meta_rows, LANES), (1, row_total)],
        "sums",
    )(place, labels.reshape(1, row_total), embeddings)
    got = exchange(payload)
    cost = pl.CostEstimate(flops=8 * row_total * width * 128, bytes_accessed=2 * row_total * width, transcendentals=row_total)
    (lengths,) = call(lengths_kernel, [VMEM], [(1, row_total)], "lengths", cost=cost)(embeddings)
    class_means, back, ids = call(
        means_kernel,
        [VMEM],
        [(CLS_DEV, width), (owner_count, slot_rows, LANES), (1, slot_total)],
        "means",
    )(got)
    units = exchange(back)
    weighted, own_similarity = call(
        weigh_kernel,
        [VMEM] * 4,
        [(owner_count, slot_rows, LANES), (1, row_total)],
        "weigh",
        scratch=[pltpu.VMEM((slot_total, width), jnp.float32)],
    )(units, embeddings, where_to, lengths)
    got_weighted = exchange(weighted)
    own = own_similarity.reshape(row_total)
    similarity = own
    for step in range(1, group_count):
        ring = [(source, (source + step) % group_count) for source in range(group_count)]
        similarity = similarity + lax.ppermute(own, "cls", ring)
    (prototypes,) = call(prototypes_kernel, [VMEM] * 2, [(CLS_DEV, width)], "prototypes")(got_weighted, ids)
    return (class_means, prototypes, similarity)


def solution(mesh):
    in_specs = (P("dp", None), P("dp"), P("dp"))
    out_specs = (P(("dp", "cls"), None), P(("dp", "cls"), None), P("dp"))
    return jax.shard_map(shards, mesh=mesh, in_specs=in_specs, out_specs=out_specs, check_vma=False)
```

```python
import functools

import jax
import jax.numpy as jnp
from jax import lax
from jax.experimental import pallas as pl
from jax.experimental.pallas import tpu as pltpu
from jax.sharding import PartitionSpec as P

CLS_DEV = 86
SLOTS = 16
LANES = 128
CLS_PAD = 96

epsilon = 1e-06
sharpness = 4.0

VMEM = pl.BlockSpec(memory_space=pltpu.VMEM)
SMEM = pl.BlockSpec(memory_space=pltpu.SMEM)
HBM = pl.BlockSpec(memory_space=pltpu.MemorySpace.HBM)
VMEM_LIMIT = 24 * 1024 * 1024
ROW_TILE = 512


def dot(a, b, dims):
    return lax.dot_general(a, b, (dims, ((), ())), preferred_element_type=jnp.float32)


def split2(x):
    hi = x.astype(jnp.bfloat16)
    lo = (x - hi.astype(jnp.float32)).astype(jnp.bfloat16)
    return hi, lo


def pick(onehot, rows, axis):
    both = jnp.concatenate([onehot, onehot], axis=axis)
    return dot(both, jnp.concatenate(split2(rows), axis=0), ((axis,), (0,)))


def flags(mask, dtype=jnp.bfloat16):
    return jnp.where(mask, 1.0, 0.0).astype(dtype)


def iota(shape, axis):
    return lax.broadcasted_iota(jnp.int32, shape, axis).astype(jnp.float32)


def put_slots(ref, rows):
    pieces = rows.shape[1] // LANES
    for owner in range(rows.shape[0] // SLOTS):
        for piece in range(pieces):
            ref[owner, piece * SLOTS:(piece + 1) * SLOTS, :] = rows[
                owner * SLOTS:(owner + 1) * SLOTS, piece * LANES:(piece + 1) * LANES
            ]


def get_slots(ref, pieces):
    rows = []
    for owner in range(ref.shape[0]):
        rows.append(
            jnp.concatenate(
                [ref[owner, piece * SLOTS:(piece + 1) * SLOTS, :] for piece in range(pieces)], axis=1
            )
        )
    return jnp.concatenate(rows, axis=0)


def fetch_rows(rows_hbm, rows_ref, row_sems, tile):
    copies = []
    for t in range(rows_ref.shape[0] // tile):
        part = pl.ds(t * tile, tile)
        copies.append(pltpu.make_async_copy(rows_hbm.at[part], rows_ref.at[part], row_sems.at[t]))
        copies[-1].start()
    return copies


def sums_kernel(group_count, place_ref, label_hbm, rows_hbm, out_ref, slot_ref, label_ref, rows_ref, label_sem, row_sems):
    owner_count = out_ref.shape[0]
    slot_total = owner_count * SLOTS
    row_total, width = rows_ref.shape
    pieces = width // LANES
    tile = min(ROW_TILE, row_total)
    label_copy = pltpu.make_async_copy(label_hbm, label_ref, label_sem)
    label_copy.start()
    row_copies = fetch_rows(rows_hbm, rows_ref, row_sems, tile)
    my_group, my_owner, live = place_ref[0], place_ref[1], place_ref[2]
    label_copy.wait()
    label = label_ref[...].astype(jnp.float32)
    block = jnp.floor((label + 0.5) * (1.0 / CLS_DEV))
    inner = label - block * CLS_DEV
    owner = jnp.floor((block + 0.5) * (1.0 / group_count))
    group = block - owner * group_count
    position = lax.broadcasted_iota(jnp.int32, (1, row_total), 1)
    owned = (group == my_group.astype(jnp.float32)) & (position < live)
    owner = jnp.where(owned, owner, -1.0)
    owner_pad = max(owner_count, 16)
    by_owner = iota((owner_pad, row_total), 0) == owner
    by_class = flags(iota((LANES, row_total), 0) == inner)
    counts = dot(flags(by_owner), by_class, ((1,), (1,)))
    present = counts > 0
    upto = flags(iota((LANES, LANES), 0) <= iota((LANES, LANES), 1))
    rank = dot(flags(present), upto, ((1,), (0,))) - 1.0
    slot = jnp.where(present, rank, -1.0)
    row_slots = dot(slot.astype(jnp.bfloat16), by_class, ((1,), (0,)))
    row_slot = jnp.sum(jnp.where(by_owner, row_slots, 0.0), axis=0, keepdims=True)
    where_to = jnp.where(owned, owner * SLOTS + row_slot, -1.0)
    slot_ref[...] = where_to
    class_at = iota((owner_pad, LANES), 1)
    lane = lax.broadcasted_iota(jnp.int32, (owner_pad, slot_total), 1) - my_owner * SLOTS
    ids = jnp.zeros((owner_pad, slot_total), jnp.float32)
    tally = jnp.zeros((owner_pad, slot_total), jnp.float32)
    for s in range(SLOTS):
        hit = slot == s
        chosen = jnp.sum(jnp.where(hit, class_at + 1.0, 0.0), axis=1, keepdims=True) - 1.0
        number = jnp.sum(jnp.where(hit, counts, 0.0), axis=1, keepdims=True)
        ids = jnp.where(lane == s, chosen, ids)
        tally = jnp.where(lane == s, number, tally)
    sub = lax.broadcasted_iota(jnp.int32, (8, LANES), 0)
    for o in range(owner_count):
        for t in range(slot_total // LANES):
            lanes = slice(t * LANES, (t + 1) * LANES)
            meta = jnp.where(sub == 0, ids[o:o + 1, lanes], jnp.where(sub == 1, tally[o:o + 1, lanes], 0.0))
            base = pieces * SLOTS + 8 * t
            out_ref[o, base:base + 8, :] = meta
    total = None
    for t in range(row_total // tile):
        part = slice(t * tile, (t + 1) * tile)
        onehot = flags(iota((slot_total, tile), 0) == where_to[:, part])
        row_copies[t].wait()
        product = dot(onehot, rows_ref[part, :], ((1,), (0,)))
        total = product if total is None else total + product
    put_slots(out_ref, total)


def means_kernel(got_ref, means_ref, back_ref, ids_ref):
    owner_count = got_ref.shape[0]
    slot_total = owner_count * SLOTS
    width = means_ref.shape[1]
    pieces = width // LANES
    metas = []
    for t in range(slot_total // LANES):
        base = pieces * SLOTS + 8 * t
        meta = got_ref[0, base:base + 8, :]
        for o in range(1, owner_count):
            meta = meta + got_ref[o, base:base + 8, :]
        metas.append(meta)
    meta = jnp.concatenate(metas, axis=1)
    ids = meta[0:1, :]
    ids_ref[...] = ids
    match = iota((CLS_PAD, slot_total), 0) == ids
    counts = jnp.sum(jnp.where(match, meta[1:2, :], 0.0), axis=1, keepdims=True)
    onehot = flags(match)
    sums = pick(onehot, get_slots(got_ref, pieces), 1)
    means = sums * (1.0 / jnp.maximum(counts, 1.0))
    means_ref[...] = means[:means_ref.shape[0]]
    unit = means * (1.0 / jnp.sqrt(jnp.sum(means * means, axis=1, keepdims=True) + epsilon))
    put_slots(back_ref, pick(onehot, unit, 0))


def lengths_kernel(rows_ref, out_ref):
    row_total, width = rows_ref.shape
    tile = min(512, row_total)
    ones = jnp.ones((16, width), jnp.bfloat16)
    for t in range(row_total // tile):
        features = rows_ref[t * tile:(t + 1) * tile, :].astype(jnp.float32)
        hi, lo = split2(features * features)
        total = dot(ones, hi, ((1,), (1,))) + dot(ones, lo, ((1,), (1,)))
        out_ref[:, t * tile:(t + 1) * tile] = jnp.sqrt(total[0:1] + epsilon)


def weigh_kernel(unit_ref, rows_hbm, slot_ref, length_ref, out_ref, sim_ref, weight_ref, rows_ref, row_sems):
    row_total, width = rows_ref.shape
    tile = min(ROW_TILE, row_total)
    row_copies = fetch_rows(rows_hbm, rows_ref, row_sems, tile)
    slot_total = out_ref.shape[0] * SLOTS
    units = jnp.concatenate(split2(get_slots(unit_ref, width // LANES)), axis=0)
    for t in range(row_total // tile):
        part = slice(t * tile, (t + 1) * tile)
        row_copies[t].wait()
        products = dot(units, rows_ref[part, :], ((1,), (1,)))
        where_to = slot_ref[:, part]
        hit = iota((slot_total, tile), 0) == where_to
        product = jnp.sum(
            jnp.where(hit, products[:slot_total] + products[slot_total:], 0.0), axis=0, keepdims=True
        )
        similarity = jnp.where(where_to >= 0, product / length_ref[:, part], 0.0)
        sim_ref[:, part] = similarity
        weight = jnp.exp(sharpness * (similarity - 1.0))
        weight_ref[:, part] = jnp.where(hit, weight, 0.0).astype(jnp.bfloat16)
    put_slots(out_ref, dot(weight_ref[...], rows_ref[...], ((1,), (0,))))


def prototypes_kernel(got_ref, ids_ref, out_ref):
    slot_total = got_ref.shape[0] * SLOTS
    onehot = flags(iota((CLS_PAD, slot_total), 0) == ids_ref[...])
    weighted = pick(onehot, get_slots(got_ref, out_ref.shape[1] // LANES), 1)
    unit = weighted * (1.0 / jnp.sqrt(jnp.sum(weighted * weighted, axis=1, keepdims=True) + epsilon))
    out_ref[...] = unit[:out_ref.shape[0]]


def call(kernel, ins, outs, name, scratch=(), cost=None):
    return pl.pallas_call(
        kernel,
        in_specs=ins,
        out_specs=[VMEM] * len(outs),
        out_shape=[
            shape if isinstance(shape, jax.ShapeDtypeStruct) else jax.ShapeDtypeStruct(shape, jnp.float32)
            for shape in outs
        ],
        scratch_shapes=list(scratch),
        compiler_params=pltpu.CompilerParams(vmem_limit_bytes=VMEM_LIMIT),
        cost_estimate=cost,
        name=name,
    )


def in_hbm(array):
    return pltpu.with_memory_space_constraint(array, pltpu.MemorySpace.HBM)


def exchange(payload):
    return lax.all_to_all(payload, "dp", split_axis=0, concat_axis=0, tiled=True)


def shards(embeddings, labels, row_count):
    row_total, width = embeddings.shape
    group_count = lax.axis_size("cls")
    owner_count = lax.axis_size("dp")
    slot_total = owner_count * SLOTS
    pieces = width // LANES
    slot_rows = pieces * SLOTS
    tiles = row_total // min(ROW_TILE, row_total)
    meta_rows = 8 * (slot_total // LANES)
    place = jnp.stack([lax.axis_index("cls"), lax.axis_index("dp"), row_count[0]]).astype(jnp.int32)
    payload, where_to = call(
        functools.partial(sums_kernel, group_count),
        [SMEM, HBM, HBM],
        [
            (owner_count, slot_rows + meta_rows, LANES),
            (1, row_total),
        ],
        "sums",
        scratch=[
            pltpu.VMEM((1, row_total), jnp.int32),
            pltpu.VMEM((row_total, width), jnp.bfloat16),
            pltpu.SemaphoreType.DMA,
            pltpu.SemaphoreType.DMA((tiles,)),
        ],
    )(place, in_hbm(labels.reshape(1, row_total)), in_hbm(embeddings))
    got = exchange(payload)
    cost = pl.CostEstimate(flops=8 * row_total * width * 128, bytes_accessed=2 * row_total * width, transcendentals=row_total)
    (lengths,) = call(lengths_kernel, [VMEM], [(1, row_total)], "lengths", cost=cost)(embeddings)
    class_means, back, ids = call(
        means_kernel,
        [VMEM],
        [(CLS_DEV, width), (owner_count, slot_rows, LANES), (1, slot_total)],
        "means",
    )(got)
    units = exchange(back)
    weighted, own_similarity = call(
        weigh_kernel,
        [VMEM, HBM, VMEM, VMEM],
        [(owner_count, slot_rows, LANES), (1, row_total)],
        "weigh",
        scratch=[
            pltpu.VMEM((slot_total, row_total), jnp.bfloat16),
            pltpu.VMEM((row_total, width), jnp.bfloat16),
            pltpu.SemaphoreType.DMA((tiles,)),
        ],
    )(units, in_hbm(embeddings), where_to, lengths)
    got_weighted = exchange(weighted)
    own = own_similarity.reshape(row_total)
    similarity = own
    for step in range(1, group_count):
        ring = [(source, (source + step) % group_count) for source in range(group_count)]
        similarity = similarity + lax.ppermute(own, "cls", ring)
    (prototypes,) = call(prototypes_kernel, [VMEM] * 2, [(CLS_DEV, width)], "prototypes")(got_weighted, ids)
    return (class_means, prototypes, similarity)


def solution(mesh):
    in_specs = (P("dp", None), P("dp"), P("dp"))
    out_specs = (P(("dp", "cls"), None), P(("dp", "cls"), None), P("dp"))
    return jax.shard_map(shards, mesh=mesh, in_specs=in_specs, out_specs=out_specs, check_vma=False)
```

```python
import functools

import jax
import jax.numpy as jnp
from jax import lax
from jax.experimental import pallas as pl
from jax.experimental.pallas import tpu as pltpu
from jax.sharding import PartitionSpec as P

CLS_DEV = 86
SLOTS = 16
LANES = 128
CLS_PAD = 96

epsilon = 1e-06
sharpness = 4.0

VMEM = pl.BlockSpec(memory_space=pltpu.VMEM)
SMEM = pl.BlockSpec(memory_space=pltpu.SMEM)
HBM = pl.BlockSpec(memory_space=pltpu.MemorySpace.HBM)
VMEM_LIMIT = 24 * 1024 * 1024


def dot(a, b, dims):
    return lax.dot_general(a, b, (dims, ((), ())), preferred_element_type=jnp.float32)


def split2(x):
    hi = x.astype(jnp.bfloat16)
    lo = (x - hi.astype(jnp.float32)).astype(jnp.bfloat16)
    return hi, lo


def pick(onehot, rows, axis):
    both = jnp.concatenate([onehot, onehot], axis=axis)
    return dot(both, jnp.concatenate(split2(rows), axis=0), ((axis,), (0,)))


def flags(mask, dtype=jnp.bfloat16):
    return jnp.where(mask, 1.0, 0.0).astype(dtype)


def iota(shape, axis):
    return lax.broadcasted_iota(jnp.int32, shape, axis).astype(jnp.float32)


def put_slots(ref, rows):
    pieces = rows.shape[1] // LANES
    for owner in range(rows.shape[0] // SLOTS):
        for piece in range(pieces):
            ref[owner, piece * SLOTS:(piece + 1) * SLOTS, :] = rows[
                owner * SLOTS:(owner + 1) * SLOTS, piece * LANES:(piece + 1) * LANES
            ]


def get_slots(ref, pieces):
    rows = []
    for owner in range(ref.shape[0]):
        rows.append(
            jnp.concatenate(
                [ref[owner, piece * SLOTS:(piece + 1) * SLOTS, :] for piece in range(pieces)], axis=1
            )
        )
    return jnp.concatenate(rows, axis=0)


def row_cuts(row_total):
    first = row_total * 2 // 3 // LANES * LANES
    return [0, first, row_total] if first else [0, row_total]


def fetch_rows(rows_hbm, rows_ref, row_sems, cuts):
    copies = []
    for t in range(len(cuts) - 1):
        part = pl.ds(cuts[t], cuts[t + 1] - cuts[t])
        copies.append(pltpu.make_async_copy(rows_hbm.at[part], rows_ref.at[part], row_sems.at[t]))
        copies[-1].start()
    return copies


def sums_kernel(group_count, place_ref, label_hbm, rows_hbm, out_ref, slot_ref, label_ref, rows_ref, label_sem, row_sems):
    owner_count = out_ref.shape[0]
    slot_total = owner_count * SLOTS
    row_total, width = rows_ref.shape
    pieces = width // LANES
    cuts = row_cuts(row_total)
    label_copy = pltpu.make_async_copy(label_hbm, label_ref, label_sem)
    label_copy.start()
    row_copies = fetch_rows(rows_hbm, rows_ref, row_sems, cuts)
    my_group, my_owner, live = place_ref[0], place_ref[1], place_ref[2]
    label_copy.wait()
    label = label_ref[...].astype(jnp.float32)
    block = jnp.floor((label + 0.5) * (1.0 / CLS_DEV))
    inner = label - block * CLS_DEV
    owner = jnp.floor((block + 0.5) * (1.0 / group_count))
    group = block - owner * group_count
    position = lax.broadcasted_iota(jnp.int32, (1, row_total), 1)
    owned = (group == my_group.astype(jnp.float32)) & (position < live)
    owner = jnp.where(owned, owner, -1.0)
    owner_pad = max(owner_count, 16)
    by_owner = iota((owner_pad, row_total), 0) == owner
    by_class = flags(iota((LANES, row_total), 0) == inner)
    counts = dot(flags(by_owner), by_class, ((1,), (1,)))
    present = counts > 0
    upto = flags(iota((LANES, LANES), 0) <= iota((LANES, LANES), 1))
    rank = dot(flags(present), upto, ((1,), (0,))) - 1.0
    slot = jnp.where(present, rank, -1.0)
    row_slots = dot(slot.astype(jnp.bfloat16), by_class, ((1,), (0,)))
    row_slot = jnp.sum(jnp.where(by_owner, row_slots, 0.0), axis=0, keepdims=True)
    where_to = jnp.where(owned, owner * SLOTS + row_slot, -1.0)
    slot_ref[...] = where_to
    class_at = iota((owner_pad, LANES), 1)
    lane = lax.broadcasted_iota(jnp.int32, (owner_pad, slot_total), 1) - my_owner * SLOTS
    ids = jnp.zeros((owner_pad, slot_total), jnp.float32)
    tally = jnp.zeros((owner_pad, slot_total), jnp.float32)
    for s in range(SLOTS):
        hit = slot == s
        chosen = jnp.sum(jnp.where(hit, class_at + 1.0, 0.0), axis=1, keepdims=True) - 1.0
        number = jnp.sum(jnp.where(hit, counts, 0.0), axis=1, keepdims=True)
        ids = jnp.where(lane == s, chosen, ids)
        tally = jnp.where(lane == s, number, tally)
    sub = lax.broadcasted_iota(jnp.int32, (8, LANES), 0)
    for o in range(owner_count):
        for t in range(slot_total // LANES):
            lanes = slice(t * LANES, (t + 1) * LANES)
            meta = jnp.where(sub == 0, ids[o:o + 1, lanes], jnp.where(sub == 1, tally[o:o + 1, lanes], 0.0))
            base = pieces * SLOTS + 8 * t
            out_ref[o, base:base + 8, :] = meta
    total = None
    for t in range(len(cuts) - 1):
        part = slice(cuts[t], cuts[t + 1])
        onehot = flags(iota((slot_total, cuts[t + 1] - cuts[t]), 0) == where_to[:, part])
        row_copies[t].wait()
        product = dot(onehot, rows_ref[part, :], ((1,), (0,)))
        total = product if total is None else total + product
    put_slots(out_ref, total)


def means_kernel(got_ref, means_ref, back_ref, ids_ref):
    owner_count = got_ref.shape[0]
    slot_total = owner_count * SLOTS
    width = means_ref.shape[1]
    pieces = width // LANES
    metas = []
    for t in range(slot_total // LANES):
        base = pieces * SLOTS + 8 * t
        meta = got_ref[0, base:base + 8, :]
        for o in range(1, owner_count):
            meta = meta + got_ref[o, base:base + 8, :]
        metas.append(meta)
    meta = jnp.concatenate(metas, axis=1)
    ids = meta[0:1, :]
    ids_ref[...] = ids
    match = iota((CLS_PAD, slot_total), 0) == ids
    counts = jnp.sum(jnp.where(match, meta[1:2, :], 0.0), axis=1, keepdims=True)
    onehot = flags(match)
    sums = pick(onehot, get_slots(got_ref, pieces), 1)
    means = sums * (1.0 / jnp.maximum(counts, 1.0))
    means_ref[...] = means[:means_ref.shape[0]]
    unit = means * (1.0 / jnp.sqrt(jnp.sum(means * means, axis=1, keepdims=True) + epsilon))
    put_slots(back_ref, pick(onehot, unit, 0))


def lengths_kernel(rows_ref, out_ref, head_ref):
    row_total, width = rows_ref.shape
    tile = min(512, row_total)
    ones = jnp.ones((16, width), jnp.bfloat16)
    head_ref[...] = rows_ref[:head_ref.shape[0], :]
    for t in range(row_total // tile):
        features = rows_ref[t * tile:(t + 1) * tile, :].astype(jnp.float32)
        hi, lo = split2(features * features)
        total = dot(ones, hi, ((1,), (1,))) + dot(ones, lo, ((1,), (1,)))
        out_ref[:, t * tile:(t + 1) * tile] = jnp.sqrt(total[0:1] + epsilon)


def weigh_kernel(unit_ref, head_ref, rows_hbm, slot_ref, length_ref, out_ref, sim_ref, weight_ref, tail_ref, tail_sem):
    head_total, width = head_ref.shape
    slot_total = out_ref.shape[0] * SLOTS
    tail_copy = pltpu.make_async_copy(rows_hbm.at[pl.ds(head_total, tail_ref.shape[0])], tail_ref, tail_sem)
    tail_copy.start()
    units = jnp.concatenate(split2(get_slots(unit_ref, width // LANES)), axis=0)
    total = None
    for rows_ref, first in ((head_ref, 0), (tail_ref, head_total)):
        part = slice(first, first + rows_ref.shape[0])
        where_to = slot_ref[:, part]
        hit = iota((slot_total, rows_ref.shape[0]), 0) == where_to
        if first:
            tail_copy.wait()
        products = dot(units, rows_ref[...], ((1,), (1,)))
        product = jnp.sum(
            jnp.where(hit, products[:slot_total] + products[slot_total:], 0.0), axis=0, keepdims=True
        )
        similarity = jnp.where(where_to >= 0, product / length_ref[:, part], 0.0)
        sim_ref[:, part] = similarity
        weight = jnp.exp(sharpness * (similarity - 1.0))
        weight_ref[:, part] = jnp.where(hit, weight, 0.0).astype(jnp.bfloat16)
        weighted = dot(weight_ref[:, part], rows_ref[...], ((1,), (0,)))
        total = weighted if total is None else total + weighted
    put_slots(out_ref, total)


def prototypes_kernel(got_ref, ids_ref, out_ref):
    slot_total = got_ref.shape[0] * SLOTS
    onehot = flags(iota((CLS_PAD, slot_total), 0) == ids_ref[...])
    weighted = pick(onehot, get_slots(got_ref, out_ref.shape[1] // LANES), 1)
    unit = weighted * (1.0 / jnp.sqrt(jnp.sum(weighted * weighted, axis=1, keepdims=True) + epsilon))
    out_ref[...] = unit[:out_ref.shape[0]]


def call(kernel, ins, outs, name, scratch=(), cost=None):
    return pl.pallas_call(
        kernel,
        in_specs=ins,
        out_specs=[VMEM] * len(outs),
        out_shape=[
            shape if isinstance(shape, jax.ShapeDtypeStruct) else jax.ShapeDtypeStruct(shape, jnp.float32)
            for shape in outs
        ],
        scratch_shapes=list(scratch),
        compiler_params=pltpu.CompilerParams(vmem_limit_bytes=VMEM_LIMIT),
        cost_estimate=cost,
        name=name,
    )


def in_hbm(array):
    return pltpu.with_memory_space_constraint(array, pltpu.MemorySpace.HBM)


def exchange(payload):
    return lax.all_to_all(payload, "dp", split_axis=0, concat_axis=0, tiled=True)


def shards(embeddings, labels, row_count):
    row_total, width = embeddings.shape
    group_count = lax.axis_size("cls")
    owner_count = lax.axis_size("dp")
    slot_total = owner_count * SLOTS
    pieces = width // LANES
    slot_rows = pieces * SLOTS
    meta_rows = 8 * (slot_total // LANES)
    place = jnp.stack([lax.axis_index("cls"), lax.axis_index("dp"), row_count[0]]).astype(jnp.int32)
    payload, where_to = call(
        functools.partial(sums_kernel, group_count),
        [SMEM, HBM, HBM],
        [
            (owner_count, slot_rows + meta_rows, LANES),
            (1, row_total),
        ],
        "sums",
        scratch=[
            pltpu.VMEM((1, row_total), jnp.int32),
            pltpu.VMEM((row_total, width), jnp.bfloat16),
            pltpu.SemaphoreType.DMA,
            pltpu.SemaphoreType.DMA((len(row_cuts(row_total)) - 1,)),
        ],
    )(place, in_hbm(labels.reshape(1, row_total)), in_hbm(embeddings))
    got = exchange(payload)
    cost = pl.CostEstimate(flops=8 * row_total * width * 128, bytes_accessed=2 * row_total * width, transcendentals=row_total)
    head = row_total // 2
    lengths, head_rows = call(
        lengths_kernel,
        [VMEM],
        [(1, row_total), jax.ShapeDtypeStruct((head, width), jnp.bfloat16)],
        "lengths",
        cost=cost,
    )(embeddings)
    class_means, back, ids = call(
        means_kernel,
        [VMEM],
        [(CLS_DEV, width), (owner_count, slot_rows, LANES), (1, slot_total)],
        "means",
    )(got)
    units = exchange(back)
    weighted, own_similarity = call(
        weigh_kernel,
        [VMEM, VMEM, HBM, VMEM, VMEM],
        [(owner_count, slot_rows, LANES), (1, row_total)],
        "weigh",
        scratch=[
            pltpu.VMEM((slot_total, row_total), jnp.bfloat16),
            pltpu.VMEM((row_total - head, width), jnp.bfloat16),
            pltpu.SemaphoreType.DMA,
        ],
    )(units, head_rows, in_hbm(embeddings), where_to, lengths)
    got_weighted = exchange(weighted)
    own = own_similarity.reshape(row_total)
    similarity = own
    for step in range(1, group_count):
        ring = [(source, (source + step) % group_count) for source in range(group_count)]
        similarity = similarity + lax.ppermute(own, "cls", ring)
    (prototypes,) = call(prototypes_kernel, [VMEM] * 2, [(CLS_DEV, width)], "prototypes")(got_weighted, ids)
    return (class_means, prototypes, similarity)


def solution(mesh):
    in_specs = (P("dp", None), P("dp"), P("dp"))
    out_specs = (P(("dp", "cls"), None), P(("dp", "cls"), None), P("dp"))
    return jax.shard_map(shards, mesh=mesh, in_specs=in_specs, out_specs=out_specs, check_vma=False)
```

```python
import functools

import jax
import jax.numpy as jnp
from jax import lax
from jax.experimental import pallas as pl
from jax.experimental.pallas import tpu as pltpu
from jax.sharding import PartitionSpec as P

CLS_DEV = 86
SLOTS = 16
LANES = 128
CLS_PAD = 96

epsilon = 1e-06
sharpness = 4.0

VMEM = pl.BlockSpec(memory_space=pltpu.VMEM)
SMEM = pl.BlockSpec(memory_space=pltpu.SMEM)
HBM = pl.BlockSpec(memory_space=pltpu.MemorySpace.HBM)
VMEM_LIMIT = 24 * 1024 * 1024


def dot(a, b, dims):
    return lax.dot_general(a, b, (dims, ((), ())), preferred_element_type=jnp.float32)


def split2(x):
    hi = x.astype(jnp.bfloat16)
    lo = (x - hi.astype(jnp.float32)).astype(jnp.bfloat16)
    return hi, lo


def pick(onehot, rows, axis):
    both = jnp.concatenate([onehot, onehot], axis=axis)
    return dot(both, jnp.concatenate(split2(rows), axis=0), ((axis,), (0,)))


def flags(mask, dtype=jnp.bfloat16):
    return jnp.where(mask, 1.0, 0.0).astype(dtype)


def iota(shape, axis):
    return lax.broadcasted_iota(jnp.int32, shape, axis).astype(jnp.float32)


def put_slots(ref, rows):
    pieces = rows.shape[1] // LANES
    for owner in range(rows.shape[0] // SLOTS):
        for piece in range(pieces):
            ref[owner, piece * SLOTS:(piece + 1) * SLOTS, :] = rows[
                owner * SLOTS:(owner + 1) * SLOTS, piece * LANES:(piece + 1) * LANES
            ]


def get_slots(ref, pieces):
    rows = []
    for owner in range(ref.shape[0]):
        rows.append(
            jnp.concatenate(
                [ref[owner, piece * SLOTS:(piece + 1) * SLOTS, :] for piece in range(pieces)], axis=1
            )
        )
    return jnp.concatenate(rows, axis=0)


def row_cuts(row_total):
    first = row_total * 2 // 3 // LANES * LANES
    return [0, first, row_total] if first else [0, row_total]


def is_early(my_group):
    return my_group % 2 == 0


def fetch_rows(rows_hbm, rows_ref, row_sems, cuts):
    copies = []
    for t in range(len(cuts) - 1):
        part = pl.ds(cuts[t], cuts[t + 1] - cuts[t])
        copies.append(pltpu.make_async_copy(rows_hbm.at[part], rows_ref.at[part], row_sems.at[t]))
        copies[-1].start()
    return copies


def sums_kernel(group_count, place_ref, label_hbm, rows_hbm, out_ref, slot_ref, length_ref, label_ref, rows_ref, label_sem, row_sems):
    owner_count = out_ref.shape[0]
    slot_total = owner_count * SLOTS
    row_total, width = rows_ref.shape
    pieces = width // LANES
    cuts = row_cuts(row_total)
    label_copy = pltpu.make_async_copy(label_hbm, label_ref, label_sem)
    label_copy.start()
    row_copies = fetch_rows(rows_hbm, rows_ref, row_sems, cuts)
    my_group, my_place, live = place_ref[0], place_ref[1], place_ref[2]
    label_copy.wait()
    label = label_ref[...].astype(jnp.float32)
    block = jnp.floor((label + 0.5) * (1.0 / CLS_DEV))
    inner = label - block * CLS_DEV
    owner = jnp.floor((block + 0.5) * (1.0 / group_count))
    group = block - owner * group_count
    position = lax.broadcasted_iota(jnp.int32, (1, row_total), 1)
    owned = (group == my_group.astype(jnp.float32)) & (position < live)
    owner = jnp.where(owned, owner, -1.0)
    owner_pad = max(owner_count, 16)
    places = lax.broadcasted_iota(jnp.int32, (owner_pad, 1), 0)
    by_owner = owner_at(places, owner_count).astype(jnp.float32) == owner
    by_class = flags(iota((LANES, row_total), 0) == inner)
    counts = dot(flags(by_owner), by_class, ((1,), (1,)))
    present = counts > 0
    upto = flags(iota((LANES, LANES), 0) <= iota((LANES, LANES), 1))
    rank = dot(flags(present), upto, ((1,), (0,))) - 1.0
    slot = jnp.where(present, rank, -1.0)
    row_slots = dot(slot.astype(jnp.bfloat16), by_class, ((1,), (0,)))
    row_slots = row_slots + (places * SLOTS).astype(jnp.float32)
    row_slot = jnp.sum(jnp.where(by_owner, row_slots, 0.0), axis=0, keepdims=True)
    where_to = jnp.where(owned, row_slot, -1.0)
    slot_ref[...] = where_to
    class_at = iota((owner_pad, LANES), 1)
    lane = lax.broadcasted_iota(jnp.int32, (owner_pad, slot_total), 1) - my_place * SLOTS
    ids = jnp.zeros((owner_pad, slot_total), jnp.float32)
    tally = jnp.zeros((owner_pad, slot_total), jnp.float32)
    for s in range(SLOTS):
        hit = slot == s
        chosen = jnp.sum(jnp.where(hit, class_at + 1.0, 0.0), axis=1, keepdims=True) - 1.0
        number = jnp.sum(jnp.where(hit, counts, 0.0), axis=1, keepdims=True)
        ids = jnp.where(lane == s, chosen, ids)
        tally = jnp.where(lane == s, number, tally)
    sub = lax.broadcasted_iota(jnp.int32, (8, LANES), 0)
    for o in range(owner_count):
        for t in range(slot_total // LANES):
            lanes = slice(t * LANES, (t + 1) * LANES)
            meta = jnp.where(sub == 0, ids[o:o + 1, lanes], jnp.where(sub == 1, tally[o:o + 1, lanes], 0.0))
            base = pieces * SLOTS + 8 * t
            out_ref[o, base:base + 8, :] = meta
    total = None
    for t in range(len(cuts) - 1):
        part = slice(cuts[t], cuts[t + 1])
        onehot = flags(iota((slot_total, cuts[t + 1] - cuts[t]), 0) == where_to[:, part])
        row_copies[t].wait()
        product = dot(onehot, rows_ref[part, :], ((1,), (0,)))
        total = product if total is None else total + product
    put_slots(out_ref, total)

    @pl.when(is_early(my_group))
    def work():
        measure_rows(rows_ref, length_ref)

    @pl.when(jnp.logical_not(is_early(my_group)))
    def later():
        length_ref[...] = jnp.zeros_like(length_ref)


def means_kernel(got_ref, means_ref, back_ref, ids_ref):
    owner_count = got_ref.shape[0]
    slot_total = owner_count * SLOTS
    width = means_ref.shape[1]
    pieces = width // LANES
    metas = []
    for t in range(slot_total // LANES):
        base = pieces * SLOTS + 8 * t
        meta = got_ref[0, base:base + 8, :]
        for o in range(1, owner_count):
            meta = meta + got_ref[o, base:base + 8, :]
        metas.append(meta)
    meta = jnp.concatenate(metas, axis=1)
    ids = meta[0:1, :]
    ids_ref[...] = ids
    match = iota((CLS_PAD, slot_total), 0) == ids
    counts = jnp.sum(jnp.where(match, meta[1:2, :], 0.0), axis=1, keepdims=True)
    onehot = flags(match)
    sums = pick(onehot, get_slots(got_ref, pieces), 1)
    means = sums * (1.0 / jnp.maximum(counts, 1.0))
    means_ref[...] = means[:means_ref.shape[0]]
    unit = means * (1.0 / jnp.sqrt(jnp.sum(means * means, axis=1, keepdims=True) + epsilon))
    put_slots(back_ref, pick(onehot, unit, 0))


def measure_rows(rows_ref, out_ref):
    row_total, width = rows_ref.shape
    tile = min(512, row_total)
    ones = jnp.ones((16, width), jnp.bfloat16)
    for t in range(row_total // tile):
        features = rows_ref[t * tile:(t + 1) * tile, :].astype(jnp.float32)
        hi, lo = split2(features * features)
        total = dot(ones, hi, ((1,), (1,))) + dot(ones, lo, ((1,), (1,)))
        out_ref[:, t * tile:(t + 1) * tile] = jnp.sqrt(total[0:1] + epsilon)


def lengths_kernel(place_ref, rows_ref, early_ref, out_ref, head_ref):
    head_ref[...] = rows_ref[:head_ref.shape[0], :]

    @pl.when(is_early(place_ref[0]))
    def take():
        out_ref[...] = early_ref[...]

    @pl.when(jnp.logical_not(is_early(place_ref[0])))
    def work():
        measure_rows(rows_ref, out_ref)


def weigh_kernel(unit_ref, head_ref, rows_hbm, slot_ref, length_ref, out_ref, sim_ref, weight_ref, tail_ref, tail_sem):
    head_total, width = head_ref.shape
    slot_total = out_ref.shape[0] * SLOTS
    tail_copy = pltpu.make_async_copy(rows_hbm.at[pl.ds(head_total, tail_ref.shape[0])], tail_ref, tail_sem)
    tail_copy.start()
    units = jnp.concatenate(split2(get_slots(unit_ref, width // LANES)), axis=0)
    total = None
    for rows_ref, first in ((head_ref, 0), (tail_ref, head_total)):
        part = slice(first, first + rows_ref.shape[0])
        where_to = slot_ref[:, part]
        hit = iota((slot_total, rows_ref.shape[0]), 0) == where_to
        if first:
            tail_copy.wait()
        products = dot(units, rows_ref[...], ((1,), (1,)))
        product = jnp.sum(
            jnp.where(hit, products[:slot_total] + products[slot_total:], 0.0), axis=0, keepdims=True
        )
        similarity = jnp.where(where_to >= 0, product / length_ref[:, part], 0.0)
        sim_ref[:, part] = similarity
        weight = jnp.exp(sharpness * (similarity - 1.0))
        weight_ref[:, part] = jnp.where(hit, weight, 0.0).astype(jnp.bfloat16)
        weighted = dot(weight_ref[:, part], rows_ref[...], ((1,), (0,)))
        total = weighted if total is None else total + weighted
    put_slots(out_ref, total)


def prototypes_kernel(got_ref, ids_ref, out_ref):
    slot_total = got_ref.shape[0] * SLOTS
    onehot = flags(iota((CLS_PAD, slot_total), 0) == ids_ref[...])
    weighted = pick(onehot, get_slots(got_ref, out_ref.shape[1] // LANES), 1)
    unit = weighted * (1.0 / jnp.sqrt(jnp.sum(weighted * weighted, axis=1, keepdims=True) + epsilon))
    out_ref[...] = unit[:out_ref.shape[0]]


def call(kernel, ins, outs, name, scratch=(), cost=None):
    return pl.pallas_call(
        kernel,
        in_specs=ins,
        out_specs=[VMEM] * len(outs),
        out_shape=[
            shape if isinstance(shape, jax.ShapeDtypeStruct) else jax.ShapeDtypeStruct(shape, jnp.float32)
            for shape in outs
        ],
        scratch_shapes=list(scratch),
        compiler_params=pltpu.CompilerParams(vmem_limit_bytes=VMEM_LIMIT),
        cost_estimate=cost,
        name=name,
    )


def in_hbm(array):
    return pltpu.with_memory_space_constraint(array, pltpu.MemorySpace.HBM)


def owner_order(owner_count):
    quarter = owner_count // 4
    if owner_count % 4:
        return list(range(owner_count))
    return [*range(2 * quarter, 3 * quarter), *range(2 * quarter), *range(3 * quarter, owner_count)]


def owner_at(place, owner_count):
    order = owner_order(owner_count)
    owner = place
    for position in range(owner_count):
        if order[position] != position:
            owner = jnp.where(place == position, order[position], owner)
    return owner


def place_of(owner, owner_count):
    place = owner
    for position, known in enumerate(owner_order(owner_count)):
        if known != position:
            place = jnp.where(owner == known, position, place)
    return place


def exchange(payload):
    order = owner_order(payload.shape[0])
    return lax.all_to_all(payload, "dp", split_axis=0, concat_axis=0, tiled=True, axis_index_groups=[order])


def shards(embeddings, labels, row_count):
    row_total, width = embeddings.shape
    group_count = lax.axis_size("cls")
    owner_count = lax.axis_size("dp")
    slot_total = owner_count * SLOTS
    pieces = width // LANES
    slot_rows = pieces * SLOTS
    meta_rows = 8 * (slot_total // LANES)
    my_place = place_of(lax.axis_index("dp"), owner_count)
    place = jnp.stack([lax.axis_index("cls"), my_place, row_count[0]]).astype(jnp.int32)
    payload, where_to, early_lengths = call(
        functools.partial(sums_kernel, group_count),
        [SMEM, HBM, HBM],
        [
            (owner_count, slot_rows + meta_rows, LANES),
            (1, row_total),
            (1, row_total),
        ],
        "sums",
        scratch=[
            pltpu.VMEM((1, row_total), jnp.int32),
            pltpu.VMEM((row_total, width), jnp.bfloat16),
            pltpu.SemaphoreType.DMA,
            pltpu.SemaphoreType.DMA((len(row_cuts(row_total)) - 1,)),
        ],
    )(place, in_hbm(labels.reshape(1, row_total)), in_hbm(embeddings))
    got = exchange(payload)
    cost = pl.CostEstimate(flops=8 * row_total * width * 128, bytes_accessed=2 * row_total * width, transcendentals=row_total)
    head = row_total // 2
    lengths, head_rows = call(
        lengths_kernel,
        [SMEM, VMEM, VMEM],
        [(1, row_total), jax.ShapeDtypeStruct((head, width), jnp.bfloat16)],
        "lengths",
        cost=cost,
    )(place, embeddings, early_lengths)
    class_means, back, ids = call(
        means_kernel,
        [VMEM],
        [(CLS_DEV, width), (owner_count, slot_rows, LANES), (1, slot_total)],
        "means",
    )(got)
    units = exchange(back)
    weighted, own_similarity = call(
        weigh_kernel,
        [VMEM, VMEM, HBM, VMEM, VMEM],
        [(owner_count, slot_rows, LANES), (1, row_total)],
        "weigh",
        scratch=[
            pltpu.VMEM((slot_total, row_total), jnp.bfloat16),
            pltpu.VMEM((row_total - head, width), jnp.bfloat16),
            pltpu.SemaphoreType.DMA,
        ],
    )(units, head_rows, in_hbm(embeddings), where_to, lengths)
    got_weighted = exchange(weighted)
    own = own_similarity.reshape(row_total)
    similarity = own
    for step in range(1, group_count):
        ring = [(source, (source + step) % group_count) for source in range(group_count)]
        similarity = similarity + lax.ppermute(own, "cls", ring)
    (prototypes,) = call(prototypes_kernel, [VMEM] * 2, [(CLS_DEV, width)], "prototypes")(got_weighted, ids)
    return (class_means, prototypes, similarity)


def solution(mesh):
    in_specs = (P("dp", None), P("dp"), P("dp"))
    out_specs = (P(("dp", "cls"), None), P(("dp", "cls"), None), P("dp"))
    return jax.shard_map(shards, mesh=mesh, in_specs=in_specs, out_specs=out_specs, check_vma=False)
```

```python
import functools

import jax
import jax.numpy as jnp
from jax import lax
from jax.experimental import pallas as pl
from jax.experimental.pallas import tpu as pltpu
from jax.sharding import PartitionSpec as P

CLS_DEV = 86
SLOTS = 16
LANES = 128
CLS_PAD = 96

epsilon = 1e-06
sharpness = 4.0

VMEM = pl.BlockSpec(memory_space=pltpu.VMEM)
HBM = pl.BlockSpec(memory_space=pltpu.MemorySpace.HBM)
VMEM_LIMIT = 24 * 1024 * 1024


def dot(a, b, dims):
    return lax.dot_general(a, b, (dims, ((), ())), preferred_element_type=jnp.float32)


def split2(x):
    hi = x.astype(jnp.bfloat16)
    lo = (x - hi.astype(jnp.float32)).astype(jnp.bfloat16)
    return hi, lo


def pick(onehot, rows, axis):
    both = jnp.concatenate([onehot, onehot], axis=axis)
    return dot(both, jnp.concatenate(split2(rows), axis=0), ((axis,), (0,)))


def flags(mask, dtype=jnp.bfloat16):
    return jnp.where(mask, 1.0, 0.0).astype(dtype)


def iota(shape, axis):
    return lax.broadcasted_iota(jnp.int32, shape, axis).astype(jnp.float32)


def put_slots(ref, rows):
    pieces = rows.shape[1] // LANES
    for owner in range(rows.shape[0] // SLOTS):
        for piece in range(pieces):
            ref[owner, piece * SLOTS:(piece + 1) * SLOTS, :] = rows[
                owner * SLOTS:(owner + 1) * SLOTS, piece * LANES:(piece + 1) * LANES
            ]


def get_slots(ref, pieces):
    rows = []
    for owner in range(ref.shape[0]):
        rows.append(
            jnp.concatenate(
                [ref[owner, piece * SLOTS:(piece + 1) * SLOTS, :] for piece in range(pieces)], axis=1
            )
        )
    return jnp.concatenate(rows, axis=0)


def row_cuts(row_total):
    first = row_total * 2 // 3 // LANES * LANES
    return [0, first, row_total] if first else [0, row_total]


def is_early(my_group):
    return my_group % 2 == 0


def fetch_rows(rows_hbm, rows_ref, row_sems, cuts):
    copies = []
    for t in range(len(cuts) - 1):
        part = pl.ds(cuts[t], cuts[t + 1] - cuts[t])
        copies.append(pltpu.make_async_copy(rows_hbm.at[part], rows_ref.at[part], row_sems.at[t]))
        copies[-1].start()
    return copies


def sums_kernel(group_count, live_ref, label_hbm, rows_hbm, out_ref, slot_ref, length_ref, label_ref, rows_ref, label_sem, row_sems):
    owner_count = out_ref.shape[0]
    slot_total = owner_count * SLOTS
    row_total, width = rows_ref.shape
    pieces = width // LANES
    cuts = row_cuts(row_total)
    label_copy = pltpu.make_async_copy(label_hbm, label_ref, label_sem)
    label_copy.start()
    row_copies = fetch_rows(rows_hbm, rows_ref, row_sems, cuts)
    my_group = lax.axis_index("cls")
    my_place = place_of(lax.axis_index("dp"), owner_count)
    live = live_ref[0]
    label_copy.wait()
    label = label_ref[...].astype(jnp.float32)
    block = jnp.floor((label + 0.5) * (1.0 / CLS_DEV))
    inner = label - block * CLS_DEV
    owner = jnp.floor((block + 0.5) * (1.0 / group_count))
    group = block - owner * group_count
    position = lax.broadcasted_iota(jnp.int32, (1, row_total), 1)
    owned = (group == my_group.astype(jnp.float32)) & (position < live)
    owner = jnp.where(owned, owner, -1.0)
    owner_pad = max(owner_count, 16)
    places = lax.broadcasted_iota(jnp.int32, (owner_pad, 1), 0)
    by_owner = owner_at(places, owner_count).astype(jnp.float32) == owner
    by_class = flags(iota((LANES, row_total), 0) == inner)
    counts = dot(flags(by_owner), by_class, ((1,), (1,)))
    present = counts > 0
    upto = flags(iota((LANES, LANES), 0) <= iota((LANES, LANES), 1))
    rank = dot(flags(present), upto, ((1,), (0,))) - 1.0
    slot = jnp.where(present, rank, -1.0)
    row_slots = dot(slot.astype(jnp.bfloat16), by_class, ((1,), (0,)))
    row_slots = row_slots + (places * SLOTS).astype(jnp.float32)
    row_slot = jnp.sum(jnp.where(by_owner, row_slots, 0.0), axis=0, keepdims=True)
    where_to = jnp.where(owned, row_slot, -1.0)
    slot_ref[...] = where_to
    total = None
    for t in range(len(cuts) - 1):
        part = slice(cuts[t], cuts[t + 1])
        onehot = flags(iota((slot_total, cuts[t + 1] - cuts[t]), 0) == where_to[:, part])
        row_copies[t].wait()
        product = dot(onehot, rows_ref[part, :], ((1,), (0,)))
        total = product if total is None else total + product
    class_at = iota((owner_pad, LANES), 1)
    lane = lax.broadcasted_iota(jnp.int32, (owner_pad, slot_total), 1) - my_place * SLOTS
    ids = jnp.zeros((owner_pad, slot_total), jnp.float32)
    tally = jnp.zeros((owner_pad, slot_total), jnp.float32)
    for s in range(SLOTS):
        hit = slot == s
        chosen = jnp.sum(jnp.where(hit, class_at + 1.0, 0.0), axis=1, keepdims=True) - 1.0
        number = jnp.sum(jnp.where(hit, counts, 0.0), axis=1, keepdims=True)
        ids = jnp.where(lane == s, chosen, ids)
        tally = jnp.where(lane == s, number, tally)
    sub = lax.broadcasted_iota(jnp.int32, (8, LANES), 0)
    for o in range(owner_count):
        for t in range(slot_total // LANES):
            lanes = slice(t * LANES, (t + 1) * LANES)
            meta = jnp.where(sub == 0, ids[o:o + 1, lanes], jnp.where(sub == 1, tally[o:o + 1, lanes], 0.0))
            base = pieces * SLOTS + 8 * t
            out_ref[o, base:base + 8, :] = meta
    put_slots(out_ref, total)

    @pl.when(is_early(my_group))
    def work():
        measure_rows(rows_ref, length_ref)

    @pl.when(jnp.logical_not(is_early(my_group)))
    def later():
        length_ref[...] = jnp.zeros_like(length_ref)


def means_kernel(got_ref, means_ref, back_ref, ids_ref):
    owner_count = got_ref.shape[0]
    slot_total = owner_count * SLOTS
    width = means_ref.shape[1]
    pieces = width // LANES
    metas = []
    for t in range(slot_total // LANES):
        base = pieces * SLOTS + 8 * t
        meta = got_ref[0, base:base + 8, :]
        for o in range(1, owner_count):
            meta = meta + got_ref[o, base:base + 8, :]
        metas.append(meta)
    meta = jnp.concatenate(metas, axis=1)
    ids = meta[0:1, :]
    ids_ref[...] = ids
    match = iota((CLS_PAD, slot_total), 0) == ids
    counts = jnp.sum(jnp.where(match, meta[1:2, :], 0.0), axis=1, keepdims=True)
    onehot = flags(match)
    sums = pick(onehot, get_slots(got_ref, pieces), 1)
    means = sums * (1.0 / jnp.maximum(counts, 1.0))
    means_ref[...] = means[:means_ref.shape[0]]
    unit = means * (1.0 / jnp.sqrt(jnp.sum(means * means, axis=1, keepdims=True) + epsilon))
    put_slots(back_ref, pick(onehot, unit, 0))


def measure_rows(rows_ref, out_ref):
    row_total, width = rows_ref.shape
    tile = min(512, row_total)
    ones = jnp.ones((16, width), jnp.bfloat16)
    for t in range(row_total // tile):
        features = rows_ref[t * tile:(t + 1) * tile, :].astype(jnp.float32)
        hi, lo = split2(features * features)
        total = dot(ones, hi, ((1,), (1,))) + dot(ones, lo, ((1,), (1,)))
        out_ref[:, t * tile:(t + 1) * tile] = jnp.sqrt(total[0:1] + epsilon)


def lengths_kernel(rows_ref, early_ref, out_ref, head_ref):
    my_group = lax.axis_index("cls")
    head_ref[...] = rows_ref[:head_ref.shape[0], :]

    @pl.when(is_early(my_group))
    def take():
        out_ref[...] = early_ref[...]

    @pl.when(jnp.logical_not(is_early(my_group)))
    def work():
        measure_rows(rows_ref, out_ref)


def weigh_kernel(unit_ref, head_ref, rows_hbm, slot_ref, length_ref, out_ref, sim_ref, weight_ref, tail_ref, tail_sem):
    head_total, width = head_ref.shape
    slot_total = out_ref.shape[0] * SLOTS
    tail_copy = pltpu.make_async_copy(rows_hbm.at[pl.ds(head_total, tail_ref.shape[0])], tail_ref, tail_sem)
    tail_copy.start()
    units = jnp.concatenate(split2(get_slots(unit_ref, width // LANES)), axis=0)

    def weights_of(rows_ref, part):
        where_to = slot_ref[:, part]
        hit = iota((slot_total, rows_ref.shape[0]), 0) == where_to
        products = dot(units, rows_ref[...], ((1,), (1,)))
        product = jnp.sum(
            jnp.where(hit, products[:slot_total] + products[slot_total:], 0.0), axis=0, keepdims=True
        )
        similarity = jnp.where(where_to >= 0, product / length_ref[:, part], 0.0)
        sim_ref[:, part] = similarity
        weight = jnp.exp(sharpness * (similarity - 1.0))
        weight_ref[:, part] = jnp.where(hit, weight, 0.0).astype(jnp.bfloat16)

    front, back = slice(0, head_total), slice(head_total, head_total + tail_ref.shape[0])
    weights_of(head_ref, front)
    tail_copy.wait()
    total = dot(weight_ref[:, front], head_ref[...], ((1,), (0,)))
    weights_of(tail_ref, back)
    put_slots(out_ref, total + dot(weight_ref[:, back], tail_ref[...], ((1,), (0,))))


def prototypes_kernel(got_ref, ids_ref, out_ref):
    slot_total = got_ref.shape[0] * SLOTS
    onehot = flags(iota((CLS_PAD, slot_total), 0) == ids_ref[...])
    weighted = pick(onehot, get_slots(got_ref, out_ref.shape[1] // LANES), 1)
    unit = weighted * (1.0 / jnp.sqrt(jnp.sum(weighted * weighted, axis=1, keepdims=True) + epsilon))
    out_ref[...] = unit[:out_ref.shape[0]]


def call(kernel, ins, outs, name, scratch=(), cost=None):
    return pl.pallas_call(
        kernel,
        in_specs=ins,
        out_specs=[VMEM] * len(outs),
        out_shape=[
            shape if isinstance(shape, jax.ShapeDtypeStruct) else jax.ShapeDtypeStruct(shape, jnp.float32)
            for shape in outs
        ],
        scratch_shapes=list(scratch),
        compiler_params=pltpu.CompilerParams(vmem_limit_bytes=VMEM_LIMIT),
        cost_estimate=cost,
        name=name,
    )


def in_hbm(array):
    return pltpu.with_memory_space_constraint(array, pltpu.MemorySpace.HBM)


def owner_order(owner_count):
    quarter = owner_count // 4
    if owner_count % 4:
        return list(range(owner_count))
    return [*range(2 * quarter, 3 * quarter), *range(2 * quarter), *range(3 * quarter, owner_count)]


def owner_at(place, owner_count):
    order = owner_order(owner_count)
    owner = place
    for position in range(owner_count):
        if order[position] != position:
            owner = jnp.where(place == position, order[position], owner)
    return owner


def place_of(owner, owner_count):
    place = owner
    for position, known in enumerate(owner_order(owner_count)):
        if known != position:
            place = jnp.where(owner == known, position, place)
    return place


def exchange(payload):
    order = owner_order(payload.shape[0])
    return lax.all_to_all(payload, "dp", split_axis=0, concat_axis=0, tiled=True, axis_index_groups=[order])


def shards(embeddings, labels, row_count):
    row_total, width = embeddings.shape
    group_count = lax.axis_size("cls")
    owner_count = lax.axis_size("dp")
    slot_total = owner_count * SLOTS
    pieces = width // LANES
    slot_rows = pieces * SLOTS
    meta_rows = 8 * (slot_total // LANES)
    payload, where_to, early_lengths = call(
        functools.partial(sums_kernel, group_count),
        [pl.BlockSpec(memory_space=pltpu.SMEM), HBM, HBM],
        [
            (owner_count, slot_rows + meta_rows, LANES),
            (1, row_total),
            (1, row_total),
        ],
        "sums",
        scratch=[
            pltpu.VMEM((1, row_total), jnp.int32),
            pltpu.VMEM((row_total, width), jnp.bfloat16),
            pltpu.SemaphoreType.DMA,
            pltpu.SemaphoreType.DMA((len(row_cuts(row_total)) - 1,)),
        ],
    )(row_count, in_hbm(labels.reshape(1, row_total)), in_hbm(embeddings))
    got = exchange(payload)
    cost = pl.CostEstimate(flops=8 * row_total * width * 128, bytes_accessed=2 * row_total * width, transcendentals=row_total)
    head = row_total * 7 // 12 // 256 * 256
    lengths, head_rows = call(
        lengths_kernel,
        [VMEM, VMEM],
        [(1, row_total), jax.ShapeDtypeStruct((head, width), jnp.bfloat16)],
        "lengths",
        cost=cost,
    )(embeddings, early_lengths)
    class_means, back, ids = call(
        means_kernel,
        [VMEM],
        [(CLS_DEV, width), (owner_count, slot_rows, LANES), (1, slot_total)],
        "means",
    )(got)
    units = exchange(back)
    weighted, own_similarity = call(
        weigh_kernel,
        [VMEM, VMEM, HBM, VMEM, VMEM],
        [(owner_count, slot_rows, LANES), (1, row_total)],
        "weigh",
        scratch=[
            pltpu.VMEM((slot_total, row_total), jnp.bfloat16),
            pltpu.VMEM((row_total - head, width), jnp.bfloat16),
            pltpu.SemaphoreType.DMA,
        ],
    )(units, head_rows, in_hbm(embeddings), where_to, lengths)
    got_weighted = exchange(weighted)
    own = own_similarity.reshape(row_total)
    similarity = own
    for step in range(1, group_count):
        ring = [(source, (source + step) % group_count) for source in range(group_count)]
        similarity = similarity + lax.ppermute(own, "cls", ring)
    (prototypes,) = call(prototypes_kernel, [VMEM] * 2, [(CLS_DEV, width)], "prototypes")(got_weighted, ids)
    return (class_means, prototypes, similarity)


def solution(mesh):
    in_specs = (P("dp", None), P("dp"), P("dp"))
    out_specs = (P(("dp", "cls"), None), P(("dp", "cls"), None), P("dp"))
    return jax.shard_map(shards, mesh=mesh, in_specs=in_specs, out_specs=out_specs, check_vma=False)
```

```python
import functools

import jax
import jax.numpy as jnp
from jax import lax
from jax.experimental import pallas as pl
from jax.experimental.pallas import tpu as pltpu
from jax.sharding import PartitionSpec as P

CLS_DEV = 86
SLOTS = 16
LANES = 128
CLS_PAD = 96

epsilon = 1e-06
sharpness = 4.0

VMEM = pl.BlockSpec(memory_space=pltpu.VMEM)
HBM = pl.BlockSpec(memory_space=pltpu.MemorySpace.HBM)
VMEM_LIMIT = 24 * 1024 * 1024


def dot(a, b, dims):
    return lax.dot_general(a, b, (dims, ((), ())), preferred_element_type=jnp.float32)


def split2(x):
    hi = x.astype(jnp.bfloat16)
    lo = (x - hi.astype(jnp.float32)).astype(jnp.bfloat16)
    return hi, lo


def pick(onehot, rows, axis):
    both = jnp.concatenate([onehot, onehot], axis=axis)
    return dot(both, jnp.concatenate(split2(rows), axis=0), ((axis,), (0,)))


def flags(mask, dtype=jnp.bfloat16):
    return jnp.where(mask, 1.0, 0.0).astype(dtype)


def iota(shape, axis):
    return lax.broadcasted_iota(jnp.int32, shape, axis).astype(jnp.float32)


def put_slots(ref, rows):
    pieces = rows.shape[1] // LANES
    for owner in range(rows.shape[0] // SLOTS):
        for piece in range(pieces):
            ref[owner, piece * SLOTS:(piece + 1) * SLOTS, :] = rows[
                owner * SLOTS:(owner + 1) * SLOTS, piece * LANES:(piece + 1) * LANES
            ]


def get_slots(ref, pieces):
    rows = []
    for owner in range(ref.shape[0]):
        rows.append(
            jnp.concatenate(
                [ref[owner, piece * SLOTS:(piece + 1) * SLOTS, :] for piece in range(pieces)], axis=1
            )
        )
    return jnp.concatenate(rows, axis=0)


def is_early(my_group):
    return my_group % 2 == 0


def sums_kernel(group_count, live_ref, label_hbm, rows_hbm, out_ref, slot_ref, length_ref, label_ref, rows_ref, label_sem, row_sem):
    owner_count = out_ref.shape[0]
    slot_total = owner_count * SLOTS
    row_total, width = rows_ref.shape
    pieces = width // LANES
    label_copy = pltpu.make_async_copy(label_hbm, label_ref, label_sem)
    label_copy.start()
    row_copy = pltpu.make_async_copy(rows_hbm, rows_ref, row_sem)
    row_copy.start()
    my_group = lax.axis_index("cls")
    my_place = place_of(lax.axis_index("dp"), owner_count)
    live = live_ref[0]
    label_copy.wait()
    label = label_ref[...].astype(jnp.float32)
    block = jnp.floor((label + 0.5) * (1.0 / CLS_DEV))
    inner = label - block * CLS_DEV
    owner = jnp.floor((block + 0.5) * (1.0 / group_count))
    group = block - owner * group_count
    position = lax.broadcasted_iota(jnp.int32, (1, row_total), 1)
    owned = (group == my_group.astype(jnp.float32)) & (position < live)
    owner = jnp.where(owned, owner, -1.0)
    owner_pad = max(owner_count, 16)
    places = lax.broadcasted_iota(jnp.int32, (owner_pad, 1), 0)
    by_owner = owner_at(places, owner_count).astype(jnp.float32) == owner
    by_class = flags(iota((LANES, row_total), 0) == inner)
    counts = dot(flags(by_owner), by_class, ((1,), (1,)))
    present = counts > 0
    upto = flags(iota((LANES, LANES), 0) <= iota((LANES, LANES), 1))
    rank = dot(flags(present), upto, ((1,), (0,))) - 1.0
    slot = jnp.where(present, rank, -1.0)
    row_slots = dot(slot.astype(jnp.bfloat16), by_class, ((1,), (0,)))
    row_slots = row_slots + (places * SLOTS).astype(jnp.float32)
    row_slot = jnp.sum(jnp.where(by_owner, row_slots, 0.0), axis=0, keepdims=True)
    where_to = jnp.where(owned, row_slot, -1.0)
    slot_ref[...] = where_to
    onehot = flags(iota((slot_total, row_total), 0) == where_to)
    row_copy.wait()
    total = dot(onehot, rows_ref[...], ((1,), (0,)))
    class_at = iota((owner_pad, LANES), 1)
    lane = lax.broadcasted_iota(jnp.int32, (owner_pad, slot_total), 1) - my_place * SLOTS
    ids = jnp.zeros((owner_pad, slot_total), jnp.float32)
    tally = jnp.zeros((owner_pad, slot_total), jnp.float32)
    for s in range(SLOTS):
        hit = slot == s
        chosen = jnp.sum(jnp.where(hit, class_at + 1.0, 0.0), axis=1, keepdims=True) - 1.0
        number = jnp.sum(jnp.where(hit, counts, 0.0), axis=1, keepdims=True)
        ids = jnp.where(lane == s, chosen, ids)
        tally = jnp.where(lane == s, number, tally)
    sub = lax.broadcasted_iota(jnp.int32, (8, LANES), 0)
    for o in range(owner_count):
        for t in range(slot_total // LANES):
            lanes = slice(t * LANES, (t + 1) * LANES)
            meta = jnp.where(sub == 0, ids[o:o + 1, lanes], jnp.where(sub == 1, tally[o:o + 1, lanes], 0.0))
            base = pieces * SLOTS + 8 * t
            out_ref[o, base:base + 8, :] = meta
    put_slots(out_ref, total)

    @pl.when(is_early(my_group))
    def work():
        measure_rows(rows_ref, length_ref)

    @pl.when(jnp.logical_not(is_early(my_group)))
    def later():
        length_ref[...] = jnp.zeros_like(length_ref)


def means_kernel(got_ref, means_ref, back_ref, ids_ref):
    owner_count = got_ref.shape[0]
    slot_total = owner_count * SLOTS
    width = means_ref.shape[1]
    pieces = width // LANES
    metas = []
    for t in range(slot_total // LANES):
        base = pieces * SLOTS + 8 * t
        meta = got_ref[0, base:base + 8, :]
        for o in range(1, owner_count):
            meta = meta + got_ref[o, base:base + 8, :]
        metas.append(meta)
    meta = jnp.concatenate(metas, axis=1)
    ids = meta[0:1, :]
    ids_ref[...] = ids
    match = iota((CLS_PAD, slot_total), 0) == ids
    counts = jnp.sum(jnp.where(match, meta[1:2, :], 0.0), axis=1, keepdims=True)
    onehot = flags(match)
    sums = pick(onehot, get_slots(got_ref, pieces), 1)
    means = sums * (1.0 / jnp.maximum(counts, 1.0))
    means_ref[...] = means[:means_ref.shape[0]]
    unit = means * (1.0 / jnp.sqrt(jnp.sum(means * means, axis=1, keepdims=True) + epsilon))
    put_slots(back_ref, pick(onehot, unit, 0))


def measure_rows(rows_ref, out_ref):
    row_total, width = rows_ref.shape
    tile = min(512, row_total)
    ones = jnp.ones((16, width), jnp.bfloat16)
    for t in range(row_total // tile):
        features = rows_ref[t * tile:(t + 1) * tile, :].astype(jnp.float32)
        hi, lo = split2(features * features)
        total = dot(ones, hi, ((1,), (1,))) + dot(ones, lo, ((1,), (1,)))
        out_ref[:, t * tile:(t + 1) * tile] = jnp.sqrt(total[0:1] + epsilon)


def lengths_kernel(rows_ref, early_ref, out_ref, head_ref):
    my_group = lax.axis_index("cls")
    head_ref[...] = rows_ref[:head_ref.shape[0], :]

    @pl.when(is_early(my_group))
    def take():
        out_ref[...] = early_ref[...]

    @pl.when(jnp.logical_not(is_early(my_group)))
    def work():
        measure_rows(rows_ref, out_ref)


def weigh_kernel(unit_ref, head_ref, rows_hbm, slot_ref, length_ref, out_ref, sim_ref, weight_ref, tail_ref, tail_sem):
    head_total, width = head_ref.shape
    slot_total = out_ref.shape[0] * SLOTS
    tail_copy = pltpu.make_async_copy(rows_hbm.at[pl.ds(head_total, tail_ref.shape[0])], tail_ref, tail_sem)
    tail_copy.start()
    units = jnp.concatenate(split2(get_slots(unit_ref, width // LANES)), axis=0)

    def weights_of(rows_ref, part):
        where_to = slot_ref[:, part]
        hit = iota((slot_total, rows_ref.shape[0]), 0) == where_to
        products = dot(units, rows_ref[...], ((1,), (1,)))
        product = jnp.sum(
            jnp.where(hit, products[:slot_total] + products[slot_total:], 0.0), axis=0, keepdims=True
        )
        similarity = jnp.where(where_to >= 0, product / length_ref[:, part], 0.0)
        sim_ref[:, part] = similarity
        weight = jnp.exp(sharpness * (similarity - 1.0))
        weight_ref[:, part] = jnp.where(hit, weight, 0.0).astype(jnp.bfloat16)

    front, back = slice(0, head_total), slice(head_total, head_total + tail_ref.shape[0])
    weights_of(head_ref, front)
    tail_copy.wait()
    total = dot(weight_ref[:, front], head_ref[...], ((1,), (0,)))
    weights_of(tail_ref, back)
    put_slots(out_ref, total + dot(weight_ref[:, back], tail_ref[...], ((1,), (0,))))


def prototypes_kernel(got_ref, ids_ref, out_ref):
    slot_total = got_ref.shape[0] * SLOTS
    onehot = flags(iota((CLS_PAD, slot_total), 0) == ids_ref[...])
    weighted = pick(onehot, get_slots(got_ref, out_ref.shape[1] // LANES), 1)
    unit = weighted * (1.0 / jnp.sqrt(jnp.sum(weighted * weighted, axis=1, keepdims=True) + epsilon))
    out_ref[...] = unit[:out_ref.shape[0]]


def call(kernel, ins, outs, name, scratch=(), cost=None):
    return pl.pallas_call(
        kernel,
        in_specs=ins,
        out_specs=[VMEM] * len(outs),
        out_shape=[
            shape if isinstance(shape, jax.ShapeDtypeStruct) else jax.ShapeDtypeStruct(shape, jnp.float32)
            for shape in outs
        ],
        scratch_shapes=list(scratch),
        compiler_params=pltpu.CompilerParams(vmem_limit_bytes=VMEM_LIMIT),
        cost_estimate=cost,
        name=name,
    )


def in_hbm(array):
    return pltpu.with_memory_space_constraint(array, pltpu.MemorySpace.HBM)


def owner_order(owner_count):
    quarter = owner_count // 4
    if owner_count % 4:
        return list(range(owner_count))
    return [*range(2 * quarter, 3 * quarter), *range(2 * quarter), *range(3 * quarter, owner_count)]


def owner_at(place, owner_count):
    order = owner_order(owner_count)
    owner = place
    for position in range(owner_count):
        if order[position] != position:
            owner = jnp.where(place == position, order[position], owner)
    return owner


def place_of(owner, owner_count):
    place = owner
    for position, known in enumerate(owner_order(owner_count)):
        if known != position:
            place = jnp.where(owner == known, position, place)
    return place


def exchange(payload):
    order = owner_order(payload.shape[0])
    return lax.all_to_all(payload, "dp", split_axis=0, concat_axis=0, tiled=True, axis_index_groups=[order])


def shards(embeddings, labels, row_count):
    row_total, width = embeddings.shape
    group_count = lax.axis_size("cls")
    owner_count = lax.axis_size("dp")
    slot_total = owner_count * SLOTS
    pieces = width // LANES
    slot_rows = pieces * SLOTS
    meta_rows = 8 * (slot_total // LANES)
    payload, where_to, early_lengths = call(
        functools.partial(sums_kernel, group_count),
        [pl.BlockSpec(memory_space=pltpu.SMEM), HBM, HBM],
        [
            (owner_count, slot_rows + meta_rows, LANES),
            (1, row_total),
            (1, row_total),
        ],
        "sums",
        scratch=[
            pltpu.VMEM((1, row_total), jnp.int32),
            pltpu.VMEM((row_total, width), jnp.bfloat16),
            pltpu.SemaphoreType.DMA,
            pltpu.SemaphoreType.DMA,
        ],
    )(row_count, in_hbm(labels.reshape(1, row_total)), in_hbm(embeddings))
    got = exchange(payload)
    cost = pl.CostEstimate(flops=8 * row_total * width * 128, bytes_accessed=2 * row_total * width, transcendentals=row_total)
    head = row_total * 7 // 12 // 256 * 256
    lengths, head_rows = call(
        lengths_kernel,
        [VMEM, VMEM],
        [(1, row_total), jax.ShapeDtypeStruct((head, width), jnp.bfloat16)],
        "lengths",
        cost=cost,
    )(embeddings, early_lengths)
    class_means, back, ids = call(
        means_kernel,
        [VMEM],
        [(CLS_DEV, width), (owner_count, slot_rows, LANES), (1, slot_total)],
        "means",
    )(got)
    units = exchange(back)
    weighted, own_similarity = call(
        weigh_kernel,
        [VMEM, VMEM, HBM, VMEM, VMEM],
        [(owner_count, slot_rows, LANES), (1, row_total)],
        "weigh",
        scratch=[
            pltpu.VMEM((slot_total, row_total), jnp.bfloat16),
            pltpu.VMEM((row_total - head, width), jnp.bfloat16),
            pltpu.SemaphoreType.DMA,
        ],
    )(units, head_rows, in_hbm(embeddings), where_to, lengths)
    got_weighted = exchange(weighted)
    own = own_similarity.reshape(row_total)
    similarity = own
    for step in range(1, group_count):
        ring = [(source, (source + step) % group_count) for source in range(group_count)]
        similarity = similarity + lax.ppermute(own, "cls", ring)
    (prototypes,) = call(prototypes_kernel, [VMEM] * 2, [(CLS_DEV, width)], "prototypes")(got_weighted, ids)
    return (class_means, prototypes, similarity)


def solution(mesh):
    in_specs = (P("dp", None), P("dp"), P("dp"))
    out_specs = (P(("dp", "cls"), None), P(("dp", "cls"), None), P("dp"))
    return jax.shard_map(shards, mesh=mesh, in_specs=in_specs, out_specs=out_specs, check_vma=False)
```

```python
import functools

import jax
import jax.numpy as jnp
from jax import lax
from jax.experimental import pallas as pl
from jax.experimental.pallas import tpu as pltpu
from jax.sharding import PartitionSpec as P

CLS_DEV = 86
SLOTS = 16
LANES = 128
CLS_PAD = 96

epsilon = 1e-06
sharpness = 4.0

VMEM = pl.BlockSpec(memory_space=pltpu.VMEM)
HBM = pl.BlockSpec(memory_space=pltpu.MemorySpace.HBM)
SHIP_PIECES = 2
EIGHTHS = (4, 6, 0, 5, 2, 3, 1, 7)
VMEM_LIMIT = 24 * 1024 * 1024


def dot(a, b, dims):
    return lax.dot_general(a, b, (dims, ((), ())), preferred_element_type=jnp.float32)


def split2(x):
    hi = x.astype(jnp.bfloat16)
    lo = (x - hi.astype(jnp.float32)).astype(jnp.bfloat16)
    return hi, lo


def pick(onehot, rows, axis):
    both = jnp.concatenate([onehot, onehot], axis=axis)
    return dot(both, jnp.concatenate(split2(rows), axis=0), ((axis,), (0,)))


def flags(mask, dtype=jnp.bfloat16):
    return jnp.where(mask, 1.0, 0.0).astype(dtype)


def iota(shape, axis):
    return lax.broadcasted_iota(jnp.int32, shape, axis).astype(jnp.float32)


def put_slots(ref, rows):
    pieces = rows.shape[1] // LANES
    for owner in range(rows.shape[0] // SLOTS):
        for piece in range(pieces):
            ref[owner, piece * SLOTS:(piece + 1) * SLOTS, :] = rows[
                owner * SLOTS:(owner + 1) * SLOTS, piece * LANES:(piece + 1) * LANES
            ]


def ship_slots(out_hbm, out_ref, out_sems, make_rows):
    owner_count, slot_rows = out_ref.shape[:2]
    step = min(SHIP_PIECES, slot_rows // SLOTS)
    copies = []
    for t in range(slot_rows // SLOTS // step):
        rows = make_rows(slice(t * step * LANES, (t + 1) * step * LANES))
        for owner in range(owner_count):
            for piece in range(step):
                first = (t * step + piece) * SLOTS
                out_ref[owner, first:first + SLOTS, :] = rows[
                    owner * SLOTS:(owner + 1) * SLOTS, piece * LANES:(piece + 1) * LANES
                ]
        part = pl.ds(t * step * SLOTS, step * SLOTS)
        copies.append(pltpu.make_async_copy(out_ref.at[:, part], out_hbm.at[:, part], out_sems.at[t]))
        copies[-1].start()
    for copy in copies:
        copy.wait()


def get_slots(ref, pieces):
    rows = []
    for owner in range(ref.shape[0]):
        rows.append(
            jnp.concatenate(
                [ref[owner, piece * SLOTS:(piece + 1) * SLOTS, :] for piece in range(pieces)], axis=1
            )
        )
    return jnp.concatenate(rows, axis=0)


def is_early(my_group):
    return my_group % 2 == 0


def sums_kernel(group_count, live_ref, label_hbm, rows_hbm, out_ref, slot_ref, length_ref, label_ref, rows_ref, label_sem, row_sem):
    owner_count = out_ref.shape[0]
    slot_total = owner_count * SLOTS
    row_total, width = rows_ref.shape
    pieces = width // LANES
    label_copy = pltpu.make_async_copy(label_hbm, label_ref, label_sem)
    label_copy.start()
    row_copy = pltpu.make_async_copy(rows_hbm, rows_ref, row_sem)
    row_copy.start()
    my_group = lax.axis_index("cls")
    my_place = place_of(lax.axis_index("dp"), owner_count)
    live = live_ref[0]
    label_copy.wait()
    label = label_ref[...].astype(jnp.float32)
    block = jnp.floor((label + 0.5) * (1.0 / CLS_DEV))
    inner = label - block * CLS_DEV
    owner = jnp.floor((block + 0.5) * (1.0 / group_count))
    group = block - owner * group_count
    position = lax.broadcasted_iota(jnp.int32, (1, row_total), 1)
    owned = (group == my_group.astype(jnp.float32)) & (position < live)
    owner = jnp.where(owned, owner, -1.0)
    owner_pad = max(owner_count, 16)
    places = lax.broadcasted_iota(jnp.int32, (owner_pad, 1), 0)
    by_owner = owner_at(places, owner_count).astype(jnp.float32) == owner
    by_class = flags(iota((LANES, row_total), 0) == inner)
    counts = dot(flags(by_owner), by_class, ((1,), (1,)))
    present = counts > 0
    upto = flags(iota((LANES, LANES), 0) <= iota((LANES, LANES), 1))
    rank = dot(flags(present), upto, ((1,), (0,))) - 1.0
    slot = jnp.where(present, rank, -1.0)
    row_slots = dot(slot.astype(jnp.bfloat16), by_class, ((1,), (0,)))
    row_slots = row_slots + (places * SLOTS).astype(jnp.float32)
    row_slot = jnp.sum(jnp.where(by_owner, row_slots, 0.0), axis=0, keepdims=True)
    where_to = jnp.where(owned, row_slot, -1.0)
    slot_ref[...] = where_to
    onehot = flags(iota((slot_total, row_total), 0) == where_to)
    row_copy.wait()
    total = dot(onehot, rows_ref[...], ((1,), (0,)))
    class_at = iota((owner_pad, LANES), 1)
    lane = lax.broadcasted_iota(jnp.int32, (owner_pad, slot_total), 1) - my_place * SLOTS
    ids = jnp.zeros((owner_pad, slot_total), jnp.float32)
    tally = jnp.zeros((owner_pad, slot_total), jnp.float32)
    for s in range(SLOTS):
        hit = slot == s
        chosen = jnp.sum(jnp.where(hit, class_at + 1.0, 0.0), axis=1, keepdims=True) - 1.0
        number = jnp.sum(jnp.where(hit, counts, 0.0), axis=1, keepdims=True)
        ids = jnp.where(lane == s, chosen, ids)
        tally = jnp.where(lane == s, number, tally)
    sub = lax.broadcasted_iota(jnp.int32, (8, LANES), 0)
    for o in range(owner_count):
        for t in range(slot_total // LANES):
            lanes = slice(t * LANES, (t + 1) * LANES)
            meta = jnp.where(sub == 0, ids[o:o + 1, lanes], jnp.where(sub == 1, tally[o:o + 1, lanes], 0.0))
            base = pieces * SLOTS + 8 * t
            out_ref[o, base:base + 8, :] = meta
    put_slots(out_ref, total)

    @pl.when(is_early(my_group))
    def work():
        measure_rows(rows_ref, length_ref)

    @pl.when(jnp.logical_not(is_early(my_group)))
    def later():
        length_ref[...] = jnp.zeros_like(length_ref)


def means_kernel(got_ref, means_ref, back_ref, ids_ref):
    owner_count = got_ref.shape[0]
    slot_total = owner_count * SLOTS
    width = means_ref.shape[1]
    pieces = width // LANES
    metas = []
    for t in range(slot_total // LANES):
        base = pieces * SLOTS + 8 * t
        meta = got_ref[0, base:base + 8, :]
        for o in range(1, owner_count):
            meta = meta + got_ref[o, base:base + 8, :]
        metas.append(meta)
    meta = jnp.concatenate(metas, axis=1)
    ids = meta[0:1, :]
    ids_ref[...] = ids
    match = iota((CLS_PAD, slot_total), 0) == ids
    counts = jnp.sum(jnp.where(match, meta[1:2, :], 0.0), axis=1, keepdims=True)
    onehot = flags(match)
    sums = pick(onehot, get_slots(got_ref, pieces), 1)
    means = sums * (1.0 / jnp.maximum(counts, 1.0))
    means_ref[...] = means[:means_ref.shape[0]]
    unit = means * (1.0 / jnp.sqrt(jnp.sum(means * means, axis=1, keepdims=True) + epsilon))
    put_slots(back_ref, pick(onehot, unit, 0))


def measure_rows(rows_ref, out_ref):
    row_total, width = rows_ref.shape
    tile = min(512, row_total)
    ones = jnp.ones((16, width), jnp.bfloat16)
    for t in range(row_total // tile):
        features = rows_ref[t * tile:(t + 1) * tile, :].astype(jnp.float32)
        hi, lo = split2(features * features)
        total = dot(ones, hi, ((1,), (1,))) + dot(ones, lo, ((1,), (1,)))
        out_ref[:, t * tile:(t + 1) * tile] = jnp.sqrt(total[0:1] + epsilon)


def lengths_kernel(rows_ref, early_ref, out_ref, head_ref):
    my_group = lax.axis_index("cls")
    head_ref[...] = rows_ref[:head_ref.shape[0], :]

    @pl.when(is_early(my_group))
    def take():
        out_ref[...] = early_ref[...]

    @pl.when(jnp.logical_not(is_early(my_group)))
    def work():
        measure_rows(rows_ref, out_ref)


def weigh_kernel(unit_ref, head_ref, rows_hbm, slot_ref, length_ref, out_hbm, sim_ref, weight_ref, tail_ref, tail_sem, out_ref, out_sems):
    head_total, width = head_ref.shape
    slot_total = out_hbm.shape[0] * SLOTS
    tail_copy = pltpu.make_async_copy(rows_hbm.at[pl.ds(head_total, tail_ref.shape[0])], tail_ref, tail_sem)
    tail_copy.start()
    units = jnp.concatenate(split2(get_slots(unit_ref, width // LANES)), axis=0)

    def weights_of(rows_ref, part):
        where_to = slot_ref[:, part]
        hit = iota((slot_total, rows_ref.shape[0]), 0) == where_to
        products = dot(units, rows_ref[...], ((1,), (1,)))
        product = jnp.sum(
            jnp.where(hit, products[:slot_total] + products[slot_total:], 0.0), axis=0, keepdims=True
        )
        similarity = jnp.where(where_to >= 0, product / length_ref[:, part], 0.0)
        sim_ref[:, part] = similarity
        weight = jnp.exp(sharpness * (similarity - 1.0))
        weight_ref[:, part] = jnp.where(hit, weight, 0.0).astype(jnp.bfloat16)

    front, back = slice(0, head_total), slice(head_total, head_total + tail_ref.shape[0])
    weights_of(head_ref, front)
    tail_copy.wait()
    weights_of(tail_ref, back)

    def weighted(lanes):
        return dot(weight_ref[:, front], head_ref[:, lanes], ((1,), (0,))) + dot(
            weight_ref[:, back], tail_ref[:, lanes], ((1,), (0,))
        )

    ship_slots(out_hbm, out_ref, out_sems, weighted)


def prototypes_kernel(got_ref, ids_ref, out_ref):
    slot_total = got_ref.shape[0] * SLOTS
    onehot = flags(iota((CLS_PAD, slot_total), 0) == ids_ref[...])
    weighted = pick(onehot, get_slots(got_ref, out_ref.shape[1] // LANES), 1)
    unit = weighted * (1.0 / jnp.sqrt(jnp.sum(weighted * weighted, axis=1, keepdims=True) + epsilon))
    out_ref[...] = unit[:out_ref.shape[0]]


def call(kernel, ins, outs, name, scratch=(), cost=None, out_specs=None):
    return pl.pallas_call(
        kernel,
        in_specs=ins,
        out_specs=out_specs or [VMEM] * len(outs),
        out_shape=[
            shape if isinstance(shape, jax.ShapeDtypeStruct) else jax.ShapeDtypeStruct(shape, jnp.float32)
            for shape in outs
        ],
        scratch_shapes=list(scratch),
        compiler_params=pltpu.CompilerParams(vmem_limit_bytes=VMEM_LIMIT),
        cost_estimate=cost,
        name=name,
    )


def in_hbm(array):
    return pltpu.with_memory_space_constraint(array, pltpu.MemorySpace.HBM)


def owner_order(owner_count):
    if owner_count % len(EIGHTHS):
        return list(range(owner_count))
    run = owner_count // len(EIGHTHS)
    return [part * run + step for part in EIGHTHS for step in range(run)]


def owner_at(place, owner_count):
    order = owner_order(owner_count)
    owner = place
    for position in range(owner_count):
        if order[position] != position:
            owner = jnp.where(place == position, order[position], owner)
    return owner


def place_of(owner, owner_count):
    place = owner
    for position, known in enumerate(owner_order(owner_count)):
        if known != position:
            place = jnp.where(owner == known, position, place)
    return place


def exchange(payload):
    order = owner_order(payload.shape[0])
    return lax.all_to_all(payload, "dp", split_axis=0, concat_axis=0, tiled=True, axis_index_groups=[order])


def shards(embeddings, labels, row_count):
    row_total, width = embeddings.shape
    group_count = lax.axis_size("cls")
    owner_count = lax.axis_size("dp")
    slot_total = owner_count * SLOTS
    pieces = width // LANES
    slot_rows = pieces * SLOTS
    meta_rows = 8 * (slot_total // LANES)
    payload, where_to, early_lengths = call(
        functools.partial(sums_kernel, group_count),
        [pl.BlockSpec(memory_space=pltpu.SMEM), HBM, HBM],
        [
            (owner_count, slot_rows + meta_rows, LANES),
            (1, row_total),
            (1, row_total),
        ],
        "sums",
        scratch=[
            pltpu.VMEM((1, row_total), jnp.int32),
            pltpu.VMEM((row_total, width), jnp.bfloat16),
            pltpu.SemaphoreType.DMA,
            pltpu.SemaphoreType.DMA,
        ],
    )(row_count, in_hbm(labels.reshape(1, row_total)), in_hbm(embeddings))
    got = exchange(payload)
    cost = pl.CostEstimate(flops=8 * row_total * width * 128, bytes_accessed=2 * row_total * width, transcendentals=row_total)
    head = row_total * 7 // 12 // 256 * 256
    lengths, head_rows = call(
        lengths_kernel,
        [VMEM, VMEM],
        [(1, row_total), jax.ShapeDtypeStruct((head, width), jnp.bfloat16)],
        "lengths",
        cost=cost,
    )(embeddings, early_lengths)
    class_means, back, ids = call(
        means_kernel,
        [VMEM],
        [(CLS_DEV, width), (owner_count, slot_rows, LANES), (1, slot_total)],
        "means",
    )(got)
    units = exchange(back)
    weighted, own_similarity = call(
        weigh_kernel,
        [VMEM, VMEM, HBM, VMEM, VMEM],
        [(owner_count, slot_rows, LANES), (1, row_total)],
        "weigh",
        scratch=[
            pltpu.VMEM((slot_total, row_total), jnp.bfloat16),
            pltpu.VMEM((row_total - head, width), jnp.bfloat16),
            pltpu.SemaphoreType.DMA,
            pltpu.VMEM((owner_count, slot_rows, LANES), jnp.float32),
            pltpu.SemaphoreType.DMA((pieces,)),
        ],
        out_specs=[HBM, VMEM],
    )(units, head_rows, in_hbm(embeddings), where_to, lengths)
    got_weighted = exchange(weighted)
    own = own_similarity.reshape(row_total)
    similarity = own
    for step in range(1, group_count):
        ring = [(source, (source + step) % group_count) for source in range(group_count)]
        similarity = similarity + lax.ppermute(own, "cls", ring)
    (prototypes,) = call(prototypes_kernel, [VMEM] * 2, [(CLS_DEV, width)], "prototypes")(got_weighted, ids)
    return (class_means, prototypes, similarity)


def solution(mesh):
    in_specs = (P("dp", None), P("dp"), P("dp"))
    out_specs = (P(("dp", "cls"), None), P(("dp", "cls"), None), P("dp"))
    return jax.shard_map(shards, mesh=mesh, in_specs=in_specs, out_specs=out_specs, check_vma=False)
```

```python
import functools

import jax
import jax.numpy as jnp
from jax import lax
from jax.experimental import pallas as pl
from jax.experimental.pallas import tpu as pltpu
from jax.sharding import PartitionSpec as P

CLS_DEV = 86
SLOTS = 16
LANES = 128
CLS_PAD = 96

epsilon = 1e-06
sharpness = 4.0

VMEM = pl.BlockSpec(memory_space=pltpu.VMEM)
HBM = pl.BlockSpec(memory_space=pltpu.MemorySpace.HBM)
SHIP_PIECES = 2
EIGHTHS = (4, 6, 0, 5, 2, 3, 1, 7)
VMEM_LIMIT = 24 * 1024 * 1024


def dot(a, b, dims):
    return lax.dot_general(a, b, (dims, ((), ())), preferred_element_type=jnp.float32)


def split2(x):
    hi = x.astype(jnp.bfloat16)
    lo = (x - hi.astype(jnp.float32)).astype(jnp.bfloat16)
    return hi, lo


def pick(onehot, rows, axis):
    both = jnp.concatenate([onehot, onehot], axis=axis)
    return dot(both, jnp.concatenate(split2(rows), axis=0), ((axis,), (0,)))


def flags(mask, dtype=jnp.bfloat16):
    return jnp.where(mask, 1.0, 0.0).astype(dtype)


def iota(shape, axis):
    return lax.broadcasted_iota(jnp.int32, shape, axis).astype(jnp.float32)


def put_slots(ref, rows):
    pieces = rows.shape[1] // LANES
    for owner in range(rows.shape[0] // SLOTS):
        for piece in range(pieces):
            ref[owner, piece * SLOTS:(piece + 1) * SLOTS, :] = rows[
                owner * SLOTS:(owner + 1) * SLOTS, piece * LANES:(piece + 1) * LANES
            ]


def ship_slots(out_hbm, out_ref, out_sems, make_rows):
    owner_count, slot_rows = out_ref.shape[:2]
    step = min(SHIP_PIECES, slot_rows // SLOTS)
    copies = []
    for t in range(slot_rows // SLOTS // step):
        rows = make_rows(slice(t * step * LANES, (t + 1) * step * LANES))
        for owner in range(owner_count):
            for piece in range(step):
                first = (t * step + piece) * SLOTS
                out_ref[owner, first:first + SLOTS, :] = rows[
                    owner * SLOTS:(owner + 1) * SLOTS, piece * LANES:(piece + 1) * LANES
                ]
        part = pl.ds(t * step * SLOTS, step * SLOTS)
        copies.append(pltpu.make_async_copy(out_ref.at[:, part], out_hbm.at[:, part], out_sems.at[t]))
        copies[-1].start()
    for copy in copies:
        copy.wait()


def get_slots(ref, pieces):
    rows = []
    for owner in range(ref.shape[0]):
        rows.append(
            jnp.concatenate(
                [ref[owner, piece * SLOTS:(piece + 1) * SLOTS, :] for piece in range(pieces)], axis=1
            )
        )
    return jnp.concatenate(rows, axis=0)


def is_early(my_group):
    return my_group % 2 == 0


def sums_kernel(group_count, live_ref, label_hbm, rows_hbm, out_ref, slot_ref, length_ref, label_ref, rows_ref, label_sem, row_sem):
    owner_count = out_ref.shape[0]
    slot_total = owner_count * SLOTS
    row_total, width = rows_ref.shape
    pieces = width // LANES
    label_copy = pltpu.make_async_copy(label_hbm, label_ref, label_sem)
    label_copy.start()
    row_copy = pltpu.make_async_copy(rows_hbm, rows_ref, row_sem)
    row_copy.start()
    my_group = lax.axis_index("cls")
    my_place = place_of(lax.axis_index("dp"), owner_count)
    live = live_ref[0]
    label_copy.wait()
    label = label_ref[...].astype(jnp.float32)
    block = jnp.floor((label + 0.5) * (1.0 / CLS_DEV))
    inner = label - block * CLS_DEV
    owner = jnp.floor((block + 0.5) * (1.0 / group_count))
    group = block - owner * group_count
    position = lax.broadcasted_iota(jnp.int32, (1, row_total), 1)
    owned = (group == my_group.astype(jnp.float32)) & (position < live)
    owner = jnp.where(owned, owner, -1.0)
    owner_pad = max(owner_count, 16)
    places = lax.broadcasted_iota(jnp.int32, (owner_pad, 1), 0)
    by_owner = owner_at(places, owner_count).astype(jnp.float32) == owner
    by_class = flags(iota((LANES, row_total), 0) == inner)
    counts = dot(flags(by_owner), by_class, ((1,), (1,)))
    present = counts > 0
    upto = flags(iota((LANES, LANES), 0) <= iota((LANES, LANES), 1))
    rank = dot(flags(present), upto, ((1,), (0,))) - 1.0
    slot = jnp.where(present, rank, -1.0)
    row_slots = dot(slot.astype(jnp.bfloat16), by_class, ((1,), (0,)))
    row_slots = row_slots + (places * SLOTS).astype(jnp.float32)
    row_slot = jnp.sum(jnp.where(by_owner, row_slots, 0.0), axis=0, keepdims=True)
    where_to = jnp.where(owned, row_slot, -1.0)
    slot_ref[...] = where_to
    onehot = flags(iota((slot_total, row_total), 0) == where_to)
    row_copy.wait()
    total = dot(onehot, rows_ref[...], ((1,), (0,)))
    class_at = iota((owner_pad, LANES), 1)
    lane = lax.broadcasted_iota(jnp.int32, (owner_pad, slot_total), 1) - my_place * SLOTS
    ids = jnp.zeros((owner_pad, slot_total), jnp.float32)
    tally = jnp.zeros((owner_pad, slot_total), jnp.float32)
    for s in range(SLOTS):
        hit = slot == s
        chosen = jnp.sum(jnp.where(hit, class_at + 1.0, 0.0), axis=1, keepdims=True) - 1.0
        number = jnp.sum(jnp.where(hit, counts, 0.0), axis=1, keepdims=True)
        ids = jnp.where(lane == s, chosen, ids)
        tally = jnp.where(lane == s, number, tally)
    sub = lax.broadcasted_iota(jnp.int32, (8, LANES), 0)
    for o in range(owner_count):
        for t in range(slot_total // LANES):
            lanes = slice(t * LANES, (t + 1) * LANES)
            meta = jnp.where(sub == 0, ids[o:o + 1, lanes], jnp.where(sub == 1, tally[o:o + 1, lanes], 0.0))
            base = pieces * SLOTS + 8 * t
            out_ref[o, base:base + 8, :] = meta
    put_slots(out_ref, total)

    @pl.when(is_early(my_group))
    def work():
        measure_rows(rows_ref, length_ref)

    @pl.when(jnp.logical_not(is_early(my_group)))
    def later():
        length_ref[...] = jnp.zeros_like(length_ref)


def mean_rows(got_ref, width):
    owner_count = got_ref.shape[0]
    slot_total = owner_count * SLOTS
    pieces = width // LANES
    metas = []
    for t in range(slot_total // LANES):
        base = pieces * SLOTS + 8 * t
        meta = got_ref[0, base:base + 8, :]
        for o in range(1, owner_count):
            meta = meta + got_ref[o, base:base + 8, :]
        metas.append(meta)
    meta = jnp.concatenate(metas, axis=1)
    ids = meta[0:1, :]
    match = iota((CLS_PAD, slot_total), 0) == ids
    counts = jnp.sum(jnp.where(match, meta[1:2, :], 0.0), axis=1, keepdims=True)
    onehot = flags(match)
    sums = pick(onehot, get_slots(got_ref, pieces), 1)
    return ids, onehot, sums * (1.0 / jnp.maximum(counts, 1.0))


def units_kernel(got_ref, back_ref, ids_ref):
    ids, onehot, means = mean_rows(got_ref, back_ref.shape[1] // SLOTS * LANES)
    ids_ref[...] = ids
    unit = means * (1.0 / jnp.sqrt(jnp.sum(means * means, axis=1, keepdims=True) + epsilon))
    put_slots(back_ref, pick(onehot, unit, 0))


def measure_rows(rows_ref, out_ref):
    row_total, width = rows_ref.shape
    tile = min(512, row_total)
    ones = jnp.ones((16, width), jnp.bfloat16)
    for t in range(row_total // tile):
        features = rows_ref[t * tile:(t + 1) * tile, :].astype(jnp.float32)
        hi, lo = split2(features * features)
        total = dot(ones, hi, ((1,), (1,))) + dot(ones, lo, ((1,), (1,)))
        out_ref[:, t * tile:(t + 1) * tile] = jnp.sqrt(total[0:1] + epsilon)


def lengths_kernel(rows_ref, early_ref, got_ref, out_ref, head_ref, means_ref):
    means_ref[...] = mean_rows(got_ref, means_ref.shape[1])[2][:means_ref.shape[0]]
    my_group = lax.axis_index("cls")
    head_ref[...] = rows_ref[:head_ref.shape[0], :]

    @pl.when(is_early(my_group))
    def take():
        out_ref[...] = early_ref[...]

    @pl.when(jnp.logical_not(is_early(my_group)))
    def work():
        measure_rows(rows_ref, out_ref)


def weigh_kernel(unit_ref, head_ref, rows_hbm, slot_ref, length_ref, out_hbm, sim_ref, weight_ref, tail_ref, tail_sem, out_ref, out_sems):
    head_total, width = head_ref.shape
    slot_total = out_hbm.shape[0] * SLOTS
    tail_copy = pltpu.make_async_copy(rows_hbm.at[pl.ds(head_total, tail_ref.shape[0])], tail_ref, tail_sem)
    tail_copy.start()
    units = jnp.concatenate(split2(get_slots(unit_ref, width // LANES)), axis=0)

    def weights_of(rows_ref, part):
        where_to = slot_ref[:, part]
        hit = iota((slot_total, rows_ref.shape[0]), 0) == where_to
        products = dot(units, rows_ref[...], ((1,), (1,)))
        product = jnp.sum(
            jnp.where(hit, products[:slot_total] + products[slot_total:], 0.0), axis=0, keepdims=True
        )
        similarity = jnp.where(where_to >= 0, product / length_ref[:, part], 0.0)
        sim_ref[:, part] = similarity
        weight = jnp.exp(sharpness * (similarity - 1.0))
        weight_ref[:, part] = jnp.where(hit, weight, 0.0).astype(jnp.bfloat16)

    front, back = slice(0, head_total), slice(head_total, head_total + tail_ref.shape[0])
    weights_of(head_ref, front)
    tail_copy.wait()
    weights_of(tail_ref, back)

    def weighted(lanes):
        return dot(weight_ref[:, front], head_ref[:, lanes], ((1,), (0,))) + dot(
            weight_ref[:, back], tail_ref[:, lanes], ((1,), (0,))
        )

    ship_slots(out_hbm, out_ref, out_sems, weighted)


def prototypes_kernel(got_ref, ids_ref, out_ref):
    slot_total = got_ref.shape[0] * SLOTS
    onehot = flags(iota((CLS_PAD, slot_total), 0) == ids_ref[...])
    weighted = pick(onehot, get_slots(got_ref, out_ref.shape[1] // LANES), 1)
    unit = weighted * (1.0 / jnp.sqrt(jnp.sum(weighted * weighted, axis=1, keepdims=True) + epsilon))
    out_ref[...] = unit[:out_ref.shape[0]]


def call(kernel, ins, outs, name, scratch=(), cost=None, out_specs=None):
    return pl.pallas_call(
        kernel,
        in_specs=ins,
        out_specs=out_specs or [VMEM] * len(outs),
        out_shape=[
            shape if isinstance(shape, jax.ShapeDtypeStruct) else jax.ShapeDtypeStruct(shape, jnp.float32)
            for shape in outs
        ],
        scratch_shapes=list(scratch),
        compiler_params=pltpu.CompilerParams(vmem_limit_bytes=VMEM_LIMIT),
        cost_estimate=cost,
        name=name,
    )


def in_hbm(array):
    return pltpu.with_memory_space_constraint(array, pltpu.MemorySpace.HBM)


def owner_order(owner_count):
    if owner_count % len(EIGHTHS):
        return list(range(owner_count))
    run = owner_count // len(EIGHTHS)
    return [part * run + step for part in EIGHTHS for step in range(run)]


def owner_at(place, owner_count):
    order = owner_order(owner_count)
    owner = place
    for position in range(owner_count):
        if order[position] != position:
            owner = jnp.where(place == position, order[position], owner)
    return owner


def place_of(owner, owner_count):
    place = owner
    for position, known in enumerate(owner_order(owner_count)):
        if known != position:
            place = jnp.where(owner == known, position, place)
    return place


def exchange(payload):
    order = owner_order(payload.shape[0])
    return lax.all_to_all(payload, "dp", split_axis=0, concat_axis=0, tiled=True, axis_index_groups=[order])


def shards(embeddings, labels, row_count):
    row_total, width = embeddings.shape
    group_count = lax.axis_size("cls")
    owner_count = lax.axis_size("dp")
    slot_total = owner_count * SLOTS
    pieces = width // LANES
    slot_rows = pieces * SLOTS
    meta_rows = 8 * (slot_total // LANES)
    payload, where_to, early_lengths = call(
        functools.partial(sums_kernel, group_count),
        [pl.BlockSpec(memory_space=pltpu.SMEM), HBM, HBM],
        [
            (owner_count, slot_rows + meta_rows, LANES),
            (1, row_total),
            (1, row_total),
        ],
        "sums",
        scratch=[
            pltpu.VMEM((1, row_total), jnp.int32),
            pltpu.VMEM((row_total, width), jnp.bfloat16),
            pltpu.SemaphoreType.DMA,
            pltpu.SemaphoreType.DMA,
        ],
    )(row_count, in_hbm(labels.reshape(1, row_total)), in_hbm(embeddings))
    got = exchange(payload)
    cost = pl.CostEstimate(flops=8 * row_total * width * 128, bytes_accessed=2 * row_total * width, transcendentals=row_total)
    head = row_total // 2
    lengths, head_rows, class_means = call(
        lengths_kernel,
        [VMEM, VMEM, VMEM],
        [(1, row_total), jax.ShapeDtypeStruct((head, width), jnp.bfloat16), (CLS_DEV, width)],
        "lengths",
        cost=cost,
    )(embeddings, early_lengths, got)
    back, ids = call(
        units_kernel,
        [VMEM],
        [(owner_count, slot_rows, LANES), (1, slot_total)],
        "units",
    )(got)
    units = exchange(back)
    weighted, own_similarity = call(
        weigh_kernel,
        [VMEM, VMEM, HBM, VMEM, VMEM],
        [(owner_count, slot_rows, LANES), (1, row_total)],
        "weigh",
        scratch=[
            pltpu.VMEM((slot_total, row_total), jnp.bfloat16),
            pltpu.VMEM((row_total - head, width), jnp.bfloat16),
            pltpu.SemaphoreType.DMA,
            pltpu.VMEM((owner_count, slot_rows, LANES), jnp.float32),
            pltpu.SemaphoreType.DMA((pieces,)),
        ],
        out_specs=[HBM, VMEM],
    )(units, head_rows, in_hbm(embeddings), where_to, lengths)
    got_weighted = exchange(weighted)
    own = own_similarity.reshape(row_total)
    similarity = own
    for step in range(1, group_count):
        ring = [(source, (source + step) % group_count) for source in range(group_count)]
        similarity = similarity + lax.ppermute(own, "cls", ring)
    (prototypes,) = call(prototypes_kernel, [VMEM] * 2, [(CLS_DEV, width)], "prototypes")(got_weighted, ids)
    return (class_means, prototypes, similarity)


def solution(mesh):
    in_specs = (P("dp", None), P("dp"), P("dp"))
    out_specs = (P(("dp", "cls"), None), P(("dp", "cls"), None), P("dp"))
    return jax.shard_map(shards, mesh=mesh, in_specs=in_specs, out_specs=out_specs, check_vma=False)
```
